32 devices in a mesh: group: 2 (over x), frame: 4 (over y, core), row: 4 (over z).
Axes of the slice: x: 2, y: 2, z: 4, core: 2. Of those that a mesh axis runs over, the one named last changes fastest.
Arguments:
- latents: bfloat16 [48, 8, 64, 320], P(('group', 'frame'), 'row'), parts along dimension 0, may hold values from -8 to 8
- condition: bfloat16 [24, 8, 64, 320], P(('group', 'frame'), 'row'), parts along dimension 0, may hold values from -6 to 6
- key_frames: int32 [24], P('group'), parts along dimension 0, may hold values from -1 to 23, as said below
- propagate: int32 [48], P('group'), parts along dimension 0, may hold values from 0 to 11, as said below
- encoder_conv: bfloat16 [9, 320, 320], replicated, may hold values from -0.109375 to 0.109375
- zero_conv: bfloat16 [320, 320], replicated, may hold values from -0.3125 to 0.3125
- attention_gain: float32 [320], replicated, may hold values from 0.25 to 1.75
- query_weight: bfloat16 [320, 320], replicated, may hold values from -3 to 3
- key_weight: bfloat16 [320, 320], replicated, may hold values from -3 to 3
- value_weight: bfloat16 [320, 320], replicated, may hold values from -0.3125 to 0.3125
- output_weight: bfloat16 [320, 320], replicated, may hold values from -0.3125 to 0.3125
- conv_gain: float32 [320], replicated, may hold values from 0.25 to 1.75
- block_conv: bfloat16 [9, 320, 320], replicated, may hold values from -0.109375 to 0.109375
Outputs:
- updated: bfloat16 [48, 8, 64, 320], P(('group', 'frame'), 'row'), parts along dimension 0
The draws below stay inside these ranges and needn't reach their ends.
There are 2 independent parts, one for each index of `group`. The reference program is written for one: setup_inputs(seed, part) draws one part's arguments, and reference() takes and returns one part's arrays. A program takes and returns all parts, laid end to end along the dimension named above; an argument that names none is the same for every part. Nothing has to cross between parts.
Inputs may be any that keep to these rules, and one draw needn't show every extreme that they name: `key_frames`: the 3 slots of index d of frame hold keyframes of frames d * 6 to (d + 1) * 6 - 1, all different, live slots first; of index d and the index half the frame axis away, one holds 3 live keyframes and the other 1. `propagate`: each frame names a live slot of its own index of frame or of an adjacent one (no wrap); a keyframe's own frame names its own slot.
All inputs are finite; a program needn't handle non-finite values.
Results may differ from the reference program's by a relative error of at most 0.014.
Values may be sent and summed in bfloat16 or wider, within the bound.
A program may use at most 64 MiB of HBM per device.

```python
import math
import jax
import jax.numpy as jnp
from jax import lax

C = 320
HEADS = 8
WIDTH = 64
FRAMES_DEV = 6
KEY_LOW = 1
KEY_SLOTS = 3
FRAMES = 24
HEIGHT = 8
KEYS = 12
N_FRAME = 4


def plan_keys(key):
    seeded = jax.random.fold_in(key, 7)
    key_busy, key_perm, key_side, key_pick = jax.random.split(seeded, 4)
    pair_count = N_FRAME // 2
    devices = jnp.arange(N_FRAME, dtype=jnp.int32)
    coin_flip = jax.random.randint(key_busy, (pair_count,), 0, 2)
    lower_half = devices < pair_count
    partner_coin = coin_flip[devices % pair_count]
    crowded = jnp.where(lower_half, partner_coin == 1, partner_coin == 0)
    live_count = jnp.where(crowded, 3 * KEY_LOW, KEY_LOW).astype(jnp.int32)
    orders = jax.vmap(lambda subkey: jax.random.permutation(subkey, FRAMES_DEV))(jax.random.split(key_perm, N_FRAME)).astype(jnp.int32)
    slot_ids = jnp.arange(KEY_SLOTS, dtype=jnp.int32)
    is_live = slot_ids[None, :] < live_count[:, None]
    key_frames = jnp.where(is_live, devices[:, None] * FRAMES_DEV + orders[:, :KEY_SLOTS], -1).reshape(-1)
    ranks_row = jnp.broadcast_to(jnp.arange(FRAMES_DEV, dtype=jnp.int32)[None, :], (N_FRAME, FRAMES_DEV))
    frame_rank = jnp.zeros((N_FRAME, FRAMES_DEV), jnp.int32).at[jnp.broadcast_to(devices[:, None], (N_FRAME, FRAMES_DEV)), orders].set(ranks_row)
    is_key = frame_rank < live_count[:, None]
    offset_side = jax.random.randint(key_side, (N_FRAME, FRAMES_DEV), -1, 2)
    offset_side = jnp.where(frame_rank == KEY_SLOTS, -1, offset_side)
    offset_side = jnp.where(frame_rank == KEY_SLOTS + 1, 1, offset_side)
    target = jnp.clip(devices[:, None] + offset_side, 0, N_FRAME - 1)
    slot_pick = jax.random.randint(key_pick, (N_FRAME, FRAMES_DEV), 0, 3 * KEY_LOW) % live_count[target]
    propagate = jnp.where(is_key, devices[:, None] * KEY_SLOTS + frame_rank, target * KEY_SLOTS + slot_pick).reshape(-1)
    return (key_frames.astype(jnp.int32), propagate.astype(jnp.int32))


def draw_key_frames(key, part):
    return plan_keys(key)[0]


def draw_propagate(key, part):
    return plan_keys(key)[1]


def draw_latents(key, part):
    full_shape = (FRAMES, HEIGHT, WIDTH, C)
    drawn = jax.random.normal(jax.random.fold_in(key, 33), full_shape, jnp.float32)
    return jnp.clip(drawn, -8.0, 8.0).astype(jnp.bfloat16)


def query_key_pair(key):
    first_weights = jax.random.normal(jax.random.fold_in(key, 43), (C, C), jnp.float32) / math.sqrt(C)
    second_weights = jax.random.normal(jax.random.fold_in(key, 44), (C, C), jnp.float32) / math.sqrt(C)
    return (jnp.clip(first_weights, -3.0, 3.0), jnp.clip(second_weights, -3.0, 3.0))


def draw_query_weight(key, part):
    return query_key_pair(key)[0].astype(jnp.bfloat16)


def draw_key_weight(key, part):
    return query_key_pair(key)[1].astype(jnp.bfloat16)


def level_of(stream_key, dims, shards, low, high):
    level = 1.0
    for position, blocks in shards:
        steps = jax.random.uniform(jax.random.fold_in(jax.random.fold_in(stream_key, 6), position), (blocks,), jnp.float32, low / len(shards), high / len(shards))
        level = level * jnp.repeat(jnp.exp(steps), dims[position] // blocks).reshape((-1,) + (1,) * (len(dims) - 1 - position))
    return level


def normal_values(own_key, shape, spread, bound, pieces=(), kind=jnp.bfloat16):
    level = level_of(own_key, shape, pieces, -0.22, 0.18) if pieces else 1.0
    array = jax.random.normal(own_key, shape, jnp.float32) * spread * level
    return jnp.minimum(jnp.maximum(array, -bound), bound).astype(kind)


def setup_inputs(seed: int = 0, part: int = 0) -> dict:
    streams_of = jax.random.split(jax.random.key(seed), 14)
    part_keys = jax.random.split(jax.random.fold_in(streams_of[13], part), 14)
    latents = draw_latents(jax.random.fold_in(jax.random.fold_in(streams_of[13], part), 71), part)
    condition = normal_values(part_keys[1], (KEYS, HEIGHT, WIDTH, C), 1.0, 6.0, ((0, 4), (1, 4)))
    key_frames = draw_key_frames(jax.random.fold_in(jax.random.fold_in(streams_of[13], part), 71), part)
    propagate = draw_propagate(jax.random.fold_in(jax.random.fold_in(streams_of[13], part), 71), part)
    encoder_conv = normal_values(streams_of[4], (9, C, C), (9 * C) ** -0.5, 0.109375)
    zero_conv = normal_values(streams_of[5], (C, C), C ** -0.5, 0.3125)
    attention_gain = jnp.clip(1.0 + 0.15 * jax.random.normal(streams_of[6], (C,), jnp.float32), 0.25, 1.75)
    query_weight = draw_query_weight(jax.random.fold_in(streams_of[13], 71), part)
    key_weight = draw_key_weight(jax.random.fold_in(streams_of[13], 71), part)
    value_weight = normal_values(streams_of[9], (C, C), C ** -0.5, 0.3125)
    output_weight = normal_values(streams_of[10], (C, C), C ** -0.5, 0.3125)
    conv_gain = jnp.clip(1.0 + 0.15 * jax.random.normal(streams_of[11], (C,), jnp.float32), 0.25, 1.75)
    block_conv = normal_values(streams_of[12], (9, C, C), (9 * C) ** -0.5, 0.109375)
    return {"latents": latents, "condition": condition, "key_frames": key_frames, "propagate": propagate, "encoder_conv": encoder_conv, "zero_conv": zero_conv, "attention_gain": attention_gain, "query_weight": query_weight, "key_weight": key_weight, "value_weight": value_weight, "output_weight": output_weight, "conv_gain": conv_gain, "block_conv": block_conv}


def convolve(images, weights):
    frame_count, row_count, col_count, channels = images.shape
    padded = jnp.pad(images, ((0, 0), (1, 1), (1, 1), (0, 0)))
    running = jnp.zeros((frame_count * row_count * col_count, weights.shape[2]), jnp.float32)
    for row_off in range(3):
        for col_off in range(3):
            window = padded[:, row_off:row_off + row_count, col_off:col_off + col_count, :].reshape(-1, channels)
            running = running + jnp.dot(window, weights[3 * row_off + col_off], preferred_element_type=jnp.float32)
    return running.reshape(frame_count, row_count, col_count, -1)

def layer_norm(values_in, scale_gain):
    average = lax.optimization_barrier(jnp.mean(values_in, axis=-1, keepdims=True))
    centered = values_in - average
    variance = lax.optimization_barrier(jnp.mean(centered * centered, axis=-1, keepdims=True))
    return centered * lax.rsqrt(variance + 1e-05) * scale_gain

def positions(frame_total, channels):
    frame_pos = jnp.arange(frame_total, dtype=jnp.float32)[:, None]
    half_index = jnp.arange(channels // 2, dtype=jnp.float32)
    frequency = jnp.exp(half_index * (-2.0 * math.log(10000.0) / channels))
    angles = frame_pos * frequency
    return jnp.stack([jnp.sin(angles), jnp.cos(angles)], axis=-1).reshape(frame_total, channels)

def reference(latents, condition, key_frames, propagate, encoder_conv, zero_conv, attention_gain, query_weight, key_weight, value_weight, output_weight, conv_gain, block_conv):
    encoded = lax.map(lambda single: jax.nn.silu(convolve(single[None], encoder_conv)[0]).astype(jnp.bfloat16), condition)
    keyres = jnp.dot(encoded.reshape(-1, C), zero_conv, preferred_element_type=jnp.float32).astype(jnp.bfloat16).reshape(encoded.shape)
    frame_ids = jnp.arange(FRAMES, dtype=jnp.int32)
    source_frame = key_frames[propagate]
    reach = jnp.exp(-jnp.abs(frame_ids - source_frame).astype(jnp.float32) / (2 * FRAMES_DEV))
    hidden = (latents.astype(jnp.float32) + reach[:, None, None, None] * keyres[propagate].astype(jnp.float32)).astype(jnp.bfloat16)
    encoding = positions(FRAMES, C)

    def attend_row(row_data):
        normed = (layer_norm(row_data.astype(jnp.float32), attention_gain) + encoding[:, None, :]).astype(jnp.bfloat16)
        flattened = normed.reshape(-1, C)
        head_shape = (FRAMES, WIDTH, HEADS, C // HEADS)
        query = jnp.dot(flattened, query_weight, preferred_element_type=jnp.float32).astype(jnp.bfloat16).reshape(head_shape)
        key_proj = jnp.dot(flattened, key_weight, preferred_element_type=jnp.float32).astype(jnp.bfloat16).reshape(head_shape)
        value_proj = jnp.dot(flattened, value_weight, preferred_element_type=jnp.float32).astype(jnp.bfloat16).reshape(head_shape)
        scores = jnp.einsum('fwhd,gwhd->whfg', query.astype(jnp.float32), key_proj.astype(jnp.float32)) / math.sqrt(C // HEADS)
        weights_soft = jax.nn.softmax(scores, axis=-1).astype(jnp.bfloat16)
        mixed_heads = jnp.einsum('whfg,gwhd->fwhd', weights_soft.astype(jnp.float32), value_proj.astype(jnp.float32)).astype(jnp.bfloat16).reshape(-1, C)
        projected = jnp.dot(mixed_heads, output_weight, preferred_element_type=jnp.float32)
        return (row_data.astype(jnp.float32).reshape(-1, C) + projected).astype(jnp.bfloat16).reshape(FRAMES, WIDTH, C)
    attended = jnp.moveaxis(lax.map(attend_row, jnp.moveaxis(hidden, 1, 0)), 0, 1)
    activated = jax.nn.silu(layer_norm(attended.astype(jnp.float32), conv_gain)).astype(jnp.bfloat16)

    def finish(pair_in):
        single_act, single_att = pair_in
        convolved = convolve(single_act[None], block_conv)[0]
        return (single_att.astype(jnp.float32) + convolved).astype(jnp.bfloat16)
    return lax.map(finish, (activated, attended))
```

```python
import functools
import math

import jax
import jax.numpy as jnp
import numpy as np
from jax import lax
from jax.experimental import pallas as pl
from jax.experimental.pallas import tpu as pltpu
from jax.sharding import PartitionSpec as P

HEADS = 8
MESH = pl.DeviceIdType.MESH
F32 = jnp.float32
BF16 = jnp.bfloat16


def positions(frame_total, channels):
    frame_pos = np.arange(frame_total, dtype=np.float64)[:, None]
    half_index = np.arange(channels // 2, dtype=np.float64)
    frequency = np.exp(half_index * (-2.0 * math.log(10000.0) / channels))
    angles = frame_pos * frequency
    stacked = np.stack([np.sin(angles), np.cos(angles)], axis=-1)
    return stacked.reshape(frame_total, channels).astype(np.float32)


def norm(values, gain):
    average = jnp.mean(values, axis=-1, keepdims=True)
    centered = values - average
    variance = jnp.mean(centered * centered, axis=-1, keepdims=True)
    return centered * lax.rsqrt(variance + 1e-05) * gain


def silu(values):
    half = 0.5 * values
    return half + half * jnp.tanh(half)


def dot(left, right):
    return jnp.dot(left, right, preferred_element_type=F32)


def dot_nt(left, right):
    return lax.dot_general(left, right, (((1,), (1,)), ((), ())), preferred_element_type=F32)


def flat(values):
    return values.astype(F32).reshape(-1, values.shape[-1]).astype(BF16)


def pack_rows(values):
    size = values.shape[1]
    whole = values.shape[2] // 128 * 128
    parts = [values[:, :, low : low + 128] for low in range(0, whole, 128)]
    tail = values[:, :, whole:]
    if size % 16 == 0:
        parts.append(jnp.concatenate([tail[:, : size // 2], tail[:, size // 2 :]], axis=2))
    else:
        parts.append(jnp.concatenate([tail, jnp.zeros_like(tail)], axis=2))
    return jnp.concatenate(parts, axis=1)


def packed_size(size, channels):
    return size * (channels // 128) + (size // 2 if size % 16 == 0 else size)


def unpack_rows(ref, index, size, channels, low, count):
    whole = channels // 128
    rest = channels - whole * 128
    def take(start, rows):
        if isinstance(index, tuple):
            return ref[index[0], :, start : start + rows].astype(F32)
        return ref[index, start : start + rows].astype(F32)

    parts = [take(i * size + low, count) for i in range(whole)]
    if size % 16:
        tail = take(whole * size + low, count)[..., :rest]
    else:
        half = size // 2
        start = low % half
        tile = take(whole * size + start, min(count, half))
        if count == size:
            tail = jnp.concatenate([tile[..., :rest], tile[..., rest:]], axis=-2)
        else:
            tail = tile[..., :rest] if low < half else tile[..., rest:]
    return jnp.concatenate(parts + [tail], axis=-1)


def pack_lead(values):
    count = values.shape[0]
    whole = values.shape[2] // 128 * 128
    parts = [values[:, :, low : low + 128] for low in range(0, whole, 128)]
    tail = values[:, :, whole:]
    parts.append(jnp.concatenate([tail[: count // 2], tail[count // 2 :]], axis=2))
    return jnp.concatenate(parts, axis=0)


def unpack_lead(values, count, channels):
    whole = channels // 128
    rest = channels - whole * 128
    parts = [values[i * count : (i + 1) * count] for i in range(whole)]
    tile = values[whole * count :]
    parts.append(jnp.concatenate([tile[..., :rest], tile[..., rest:]], axis=0))
    return jnp.concatenate(parts, axis=-1)


def pack_tails(tails, packed, main):
    wide = 3 * main
    for a in range(3):
        parts = [tails[3 * a + b] for b in range(3)]
        packed[a, :, wide:] = jnp.concatenate(parts, axis=1)


def conv_local(images, packed, put, add):
    rows = images.shape[1]
    put(slice(0, rows), dot(flat(images), packed[1]))
    if rows > 1:
        add(slice(1, rows), dot(flat(images[:, : rows - 1]), packed[0]))
        add(slice(0, rows - 1), dot(flat(images[:, 1:]), packed[2]))


def pair_tiles(weight, width):
    rows, channels = weight.shape
    tiles = []
    for low in range(0, channels, width):
        tiles.append(weight[:, low : low + width])
        tiles.append(jnp.zeros((rows, 128 - width), weight.dtype))
    return jnp.concatenate(tiles, axis=1)


def conv_row(total, main, tail):
    cols = total.shape[0]
    col = lax.broadcasted_iota(jnp.int32, (cols, 1), 0)
    pieces = []
    for start, size in ((0, main), (3 * main, tail)):
        left, middle, right = (total[:, start + b * size : start + (b + 1) * size] for b in range(3))
        left = jnp.where(col == 0, 0.0, pltpu.roll(left, 1, 0))
        right = jnp.where(col == cols - 1, 0.0, pltpu.roll(right, cols - 1, 0))
        pieces.append(left + middle + right)
    return jnp.concatenate(pieces, axis=1)


def kernel(
    n,
    row_total,
    lat,
    cond_hbm,
    key_hbm,
    prop_hbm,
    encoding_hbm,
    gain_a_hbm,
    gain_c_hbm,
    enc_hbm,
    zero_hbm,
    q_hbm,
    k_hbm,
    v_hbm,
    o_hbm,
    blk_hbm,
    out,
    key_frames,
    propagate,
    encoding,
    gain_a,
    gain_c,
    cond,
    enc_w,
    enc_t,
    zero_w,
    q_w,
    k_w,
    v_w,
    o_w,
    blk_w,
    blk_t,
    v_wt,
    q_wp,
    k_wp,
    q_both,
    k_held,
    v_held,
    scores,
    probs,
    mixed_t,
    lat_own,
    lat_out,
    lat_pix,
    res_out,
    res_pix,
    hidden,
    att_out,
    att_in,
    att,
    act,
    cond_out,
    cond_top,
    cond_bot,
    act_out,
    act_top,
    act_bot,
    sums_e,
    sums_b,
    w_sem,
    send,
    lat_recv,
    res_recv,
    att_recv,
    ch_recv,
    ah_recv,
):
    me = lax.axis_index("frame")
    row_me = lax.axis_index("row")
    frames_dev, _, pix, channels = lat.shape
    slots, rows, cols, _ = cond.shape
    chunks = res_recv.shape[0]
    chunk = pix // chunks
    frames = hidden.shape[0]
    pieces, group = att.shape[2:4]
    per_chunk = chunk // group
    per_row = n // rows
    head_dim = channels // HEADS
    main = enc_w.shape[2] // 3 // 128 * 128
    tail = channels - main
    has_up = row_me > 0
    has_down = row_me < row_total - 1

    barrier = pltpu.get_barrier_semaphore()
    for k in range(1, n):
        pl.semaphore_signal(
            barrier, inc=1, device_id={"frame": lax.rem(me + k, n)}, device_id_type=MESH
        )

    @pl.when(has_up)
    def _():
        pl.semaphore_signal(barrier, inc=1, device_id={"row": row_me - 1}, device_id_type=MESH)

    @pl.when(has_down)
    def _():
        pl.semaphore_signal(barrier, inc=1, device_id={"row": row_me + 1}, device_id_type=MESH)

    def start_taps(src, packed, sem):
        for a in range(3):
            for b in range(3):
                pltpu.make_async_copy(
                    src.at[3 * a + b, :, :main], packed.at[a, :, b * main : (b + 1) * main], sem
                ).start()

    def wait_taps(packed, sem):
        whole = packed.at[:, :, : 3 * main]
        pltpu.make_async_copy(whole, whole, sem).wait()

    pairs = [
        (cond_hbm, cond),
        (enc_hbm.at[:, :, main:], enc_t),
        (v_hbm, v_w),
        (zero_hbm, zero_w),
        (q_hbm, q_w),
        (k_hbm, k_w),
        (o_hbm, o_w),
        (encoding_hbm, encoding),
        (gain_a_hbm, gain_a),
        (gain_c_hbm, gain_c),
        (key_hbm, key_frames),
        (prop_hbm, propagate),
        (blk_hbm.at[:, :, main:], blk_t),
        (lat, lat_own),
    ]
    loads = [pltpu.make_async_copy(s, d, w_sem.at[2 + i]) for i, (s, d) in enumerate(pairs)]
    loads[0].start()
    loads[13].start()
    loads[1].start()
    start_taps(enc_hbm, enc_w, w_sem.at[0])

    @pl.when(jnp.logical_not(has_up))
    def _():
        cond_top[...] = jnp.zeros_like(cond_top)
        act_top[...] = jnp.zeros_like(act_top)

    @pl.when(jnp.logical_not(has_down))
    def _():
        cond_bot[...] = jnp.zeros_like(cond_bot)
        act_bot[...] = jnp.zeros_like(act_bot)

    loads[0].wait()
    cond_out[0] = pack_rows(cond[:, 0].astype(F32)).astype(BF16)
    cond_out[1] = pack_rows(cond[:, rows - 1].astype(F32)).astype(BF16)
    loads[13].wait()
    for p in range(n):
        lat_out[p] = pack_rows(lat_own[:, p].astype(F32)).astype(BF16)

    neighbours = has_up.astype(jnp.int32) + has_down.astype(jnp.int32)
    with jax.named_scope("w_barrier"):
        pl.semaphore_wait(barrier, n - 1 + neighbours)

    def remote(src, dst, send_sem, recv_sem, **where):
        return pltpu.make_async_remote_copy(
            src_ref=src,
            dst_ref=dst,
            send_sem=send_sem,
            recv_sem=recv_sem,
            device_id=where,
            device_id_type=MESH,
        )

    def up(src, dst, send_sem, recv_sem):
        return remote(src, dst, send_sem, recv_sem, row=row_me - 1)

    def down(src, dst, send_sem, recv_sem):
        return remote(src, dst, send_sem, recv_sem, row=row_me + 1)

    def drain(ref, sem):
        pltpu.make_async_copy(ref, ref, sem).wait()

    cond_up = up(cond_out.at[0], cond_bot, send.at[0], ch_recv.at[0])
    cond_down = down(cond_out.at[1], cond_top, send.at[1], ch_recv.at[1])
    pl.when(has_up)(cond_up.start)
    pl.when(has_down)(cond_down.start)

    peers = [lax.rem(me + k, n) for k in range(1, n)]
    for peer in peers:
        remote(
            lat_out.at[peer],
            lat_pix.at[pl.ds(me * frames_dev, frames_dev)],
            send.at[2],
            lat_recv.at[0],
            frame=peer,
        ).start()
    lat_pix[pl.ds(me * frames_dev, frames_dev)] = lat_out[me]
    for load in loads[2:13]:
        load.start()
    start_taps(blk_hbm, blk_w, w_sem.at[1])

    with jax.named_scope("w_load01"):
        loads[1].wait()
    with jax.named_scope("pack_enc"):
        pack_tails(enc_t, enc_w, main)
        wait_taps(enc_w, w_sem.at[0])

    def edge_rows(ref, index, size):
        values = unpack_rows(ref, index, size, channels, 0, size)
        return values.reshape(-1, channels).astype(BF16)

    def put_e(r, value):
        sums_e[:, r] = value.reshape(slots, -1, cols, value.shape[-1])

    def add_e(r, value):
        sums_e[:, r] += value.reshape(slots, -1, cols, value.shape[-1])

    with jax.named_scope("encconv_local"):
        conv_local(cond[...], enc_w, put_e, add_e)
    with jax.named_scope("prep"):
        loads[2].wait()
        v_wt[...] = jnp.transpose(v_w[...].astype(F32)).astype(BF16)
        for load in loads[4:6]:
            load.wait()
        q_wp[...] = pair_tiles(q_w[...], 2 * head_dim)
        k_wp[...] = pair_tiles(k_w[...], 2 * head_dim)
        loads[12].wait()
        pack_tails(blk_t, blk_w, main)
    with jax.named_scope("w_condhalo"):
        pl.when(has_up)(cond_down.wait_recv)
        pl.when(has_down)(cond_up.wait_recv)
    with jax.named_scope("encconv_edge"):
        add_e(slice(0, 1), dot(edge_rows(cond_top, slice(None), cols), enc_w[0]))
        add_e(slice(rows - 1, rows), dot(edge_rows(cond_bot, slice(None), cols), enc_w[2]))
    with jax.named_scope("enc_silu_zero"):
        loads[3].wait()
        encoded = jnp.concatenate(
            [silu(conv_row(sums_e[s, r], main, tail)) for s in range(slots) for r in range(rows)],
            axis=0,
        ).astype(BF16)
        keyres = dot(encoded, zero_w[...]).reshape(slots, n, pix, channels)
        for p in range(n):
            for c in range(chunks):
                part = pack_rows(keyres[:, p, c * chunk : (c + 1) * chunk])
                res_out[p, c] = part.astype(BF16)
    for c in range(chunks):
        for peer in peers:
            remote(
                res_out.at[peer, c],
                res_pix[c].at[pl.ds(me * slots, slots)],
                send.at[3],
                res_recv.at[c],
                frame=peer,
            ).start()
    for c in range(chunks):
        res_pix[c][pl.ds(me * slots, slots)] = res_out[me, c]

    with jax.named_scope("w_loads"):
        for load in loads[6:12]:
            load.wait()
    with jax.named_scope("w_lat"):
        drain(lat_pix.at[: (n - 1) * frames_dev], lat_recv.at[0])

    small = frames <= 24
    block = frames * group
    factor = math.log2(math.e) / math.sqrt(head_dim)
    encode = encoding[...][:, None, :]
    lane = lax.broadcasted_iota(jnp.int32, (1, 128), 1)
    pairs_total = HEADS // 2

    def soft(values):
        width = values.shape[-1]
        values = values.reshape(frames, group, width)
        top = jnp.max(values, axis=0, keepdims=True)
        powers = jnp.exp2(values - top)
        total = jnp.sum(powers, axis=0, keepdims=True)
        pixel = lax.broadcasted_iota(jnp.int32, (1, group, width), 1)
        query = lax.broadcasted_iota(jnp.int32, (1, group, width), 2)
        weight = jnp.where(lax.rem(query, group) == pixel, 1.0 / total, 0.0)
        return (powers * weight).reshape(block, width).astype(BF16)

    def hide(c):
        span = slice(c * chunk, (c + 1) * chunk)
        drain(res_pix[c].at[: (n - 1) * slots], res_recv.at[c])

        def one(f, carry):
            slot = propagate[f]
            gap = jnp.abs(f - key_frames[slot]).astype(F32)
            reach = jnp.exp(jnp.full((1, channels), -gap / (2 * frames_dev), F32))
            residual = unpack_rows(res_pix[c], slot, chunk, channels, 0, chunk)
            value = unpack_rows(lat_pix, f, pix, channels, c * chunk, chunk) + reach * residual
            hidden[f, span] = value.astype(BF16).astype(F32)
            return carry

        lax.fori_loop(0, frames, one, 0, unroll=small)

    def project(s):
        if s % per_chunk == 0:
            hide(s // per_chunk)
        base = hidden[:, s * group : (s + 1) * group]
        normed = (norm(base, gain_a[...]) + encode).reshape(block, channels).astype(BF16)
        query = dot(normed, q_wp[...]) * factor
        for j in range(pairs_total):
            tile = query[:, 128 * j : 128 * (j + 1)]
            q_both[s % 2, j, :block] = jnp.where(lane < head_dim, tile, 0.0).astype(BF16)
            q_both[s % 2, j, block:] = jnp.where(lane < head_dim, 0.0, tile).astype(BF16)
        k_held[s % 2] = dot(normed, k_wp[...]).astype(BF16)
        v_held[s % 2] = dot_nt(v_wt[...], normed).astype(BF16)

    def score(s, j):
        keys = k_held[s % 2, :, 128 * j : 128 * (j + 1)]
        scores[j % 2] = dot_nt(keys, q_both[s % 2, j])

    def soften(s, j):
        probs[j % 2] = soft(scores[j % 2])

    def mix(s, j):
        low, high = 2 * j * head_dim, 2 * (j + 1) * head_dim
        pair = dot(v_held[s % 2, low:high], probs[j % 2])
        mixed_t[low : low + head_dim] = pair[:head_dim, :block]
        mixed_t[low + head_dim : high] = pair[head_dim:, block:]

    def finish(s):
        mixed = jnp.transpose(mixed_t[...]).astype(BF16)
        projected = dot(mixed, o_w[...]).reshape(frames, group, channels)
        base = hidden[:, s * group : (s + 1) * group]
        total = base + projected
        for p in range(n):
            part = pack_lead(total[p * frames_dev : (p + 1) * frames_dev])
            att_out[s, p] = part.astype(BF16)
        for peer in peers:
            remote(
                att_out.at[s, peer],
                att_in.at[me, s],
                send.at[4],
                att_recv.at[s],
                frame=peer,
            ).start()
        att_in[me, s] = att_out[s, me]

    with jax.named_scope("attention"):
        if small:
            steps = [(s, j) for s in range(pieces) for j in range(pairs_total)]
            project(0)
            score(*steps[0])
            for k, (s, j) in enumerate(steps):
                if k + 1 < len(steps):
                    score(*steps[k + 1])
                soften(s, j)
                if k > 0:
                    mix(*steps[k - 1])
                    if steps[k - 1][1] == pairs_total - 1:
                        finish(steps[k - 1][0])
                if j == 1 and s + 1 < pieces:
                    project(s + 1)
            mix(*steps[-1])
            finish(pieces - 1)
        else:
            for s in range(pieces):
                project(s)

                def step(j, carry):
                    keys = k_held[s % 2, :, pl.ds(pl.multiple_of(128 * j, 128), 128)]
                    for i in range(2):
                        part = q_both[s % 2, j, i * block : (i + 1) * block]
                        row = pl.ds(pl.multiple_of((2 * j + i) * head_dim, 8), head_dim)
                        value = dot(v_held[s % 2], soft(dot_nt(keys, part)))
                        scores[0, :channels, :block] = value
                        mixed_t[row] = scores[0, row, :block]
                    return carry

                lax.fori_loop(0, pairs_total, step, 0)
                finish(s)

    def add_b(r, span, ref, taps):
        parts = [edge_rows(ref, (s,), per_row * group) for s in range(span.start, span.stop)]
        value = dot(jnp.concatenate(parts, axis=0), taps)
        value = value.reshape(len(parts), frames_dev, per_row, group, value.shape[-1])
        for i, s in enumerate(range(span.start, span.stop)):
            sums_b[:, r, :, s] += value[i]

    def put_all(r, value):
        sums_b[:, r] = value.reshape(frames_dev, -1, per_row, pieces, group, value.shape[-1])

    def add_all(r, value):
        sums_b[:, r] += value.reshape(frames_dev, -1, per_row, pieces, group, value.shape[-1])

    act_ups, act_downs = [], []
    for s in range(pieces):
        with jax.named_scope(f"w_att{s}"):
            drain(att_in.at[: n - 1, s], att_recv.at[s])
        with jax.named_scope(f"act{s}"):
            taken = [unpack_lead(att_in[p, s].astype(F32), frames_dev, channels) for p in range(n)]
            value = jnp.stack(taken, axis=1)
            att[:, :, s] = value.astype(BF16)
            value = silu(norm(value, gain_c[...])).reshape(frames_dev, rows, -1, channels)
            act_out[0, s] = pack_rows(value[:, 0]).astype(BF16)
            act_out[1, s] = pack_rows(value[:, rows - 1]).astype(BF16)
            value = value.reshape(frames_dev, rows, per_row, group, channels)
            act[:, :, :, s] = value.astype(BF16)
        act_up = up(act_out.at[0, s], act_bot.at[s], send.at[5], ah_recv.at[0, s])
        act_down = down(
            act_out.at[1, s], act_top.at[s], send.at[6], ah_recv.at[1, s]
        )
        pl.when(has_up)(act_up.start)
        pl.when(has_down)(act_down.start)
        act_ups.append(act_up)
        act_downs.append(act_down)
    wait_taps(blk_w, w_sem.at[1])
    with jax.named_scope("blkconv_local"):
        conv_local(act[...].reshape(frames_dev, rows, -1, group, channels), blk_w, put_all, add_all)
    last = max(pieces - 1, 0)
    for span in [slice(0, last), slice(last, pieces)] if last else [slice(0, pieces)]:
        with jax.named_scope(f"w_acthalo{span.start}"):
            for s in range(span.start, span.stop):
                pl.when(has_up)(act_downs[s].wait_recv)
                pl.when(has_down)(act_ups[s].wait_recv)
        with jax.named_scope(f"blkconv_edge{span.start}"):
            add_b(0, span, act_top, blk_w[0])
            add_b(rows - 1, span, act_bot, blk_w[2])
    with jax.named_scope("final"):
        for f in range(frames_dev):
            for r in range(rows):
                convolved = conv_row(sums_b[f, r].reshape(cols, -1), main, tail)
                held = att[f, r * per_row : (r + 1) * per_row].astype(F32).reshape(cols, channels)
                out[f, r] = (held + convolved).astype(BF16)
    with jax.named_scope("w_end"):
        pl.when(has_up)(cond_up.wait_send)
        pl.when(has_down)(cond_down.wait_send)
        drain(lat_pix.at[: (n - 1) * frames_dev], send.at[2])
        drain(res_out.at[: n - 1], send.at[3])
        drain(att_out.at[:, : n - 1], send.at[4])
        pl.when(has_up)(lambda: drain(act_out.at[0], send.at[5]))
        pl.when(has_down)(lambda: drain(act_out.at[1], send.at[6]))


def shards(
    latents,
    condition,
    key_frames,
    propagate,
    encoder_conv,
    zero_conv,
    attention_gain,
    query_weight,
    key_weight,
    value_weight,
    output_weight,
    conv_gain,
    block_conv,
):
    frames_dev, rows, cols, channels = latents.shape
    slots = condition.shape[0]
    n = lax.axis_size("frame")
    row_total = lax.axis_size("row")
    pix = rows * cols // n
    frames = frames_dev * n
    chunk = 16 if pix % 16 == 0 else 8
    chunks = pix // chunk
    group = 8
    pieces = pix // group
    block = frames * group
    per_row = n // rows
    main = channels // 256 * 256
    tail = channels - main
    wide = 3 * (main + tail)
    lat_size = packed_size(pix, channels)
    res_size = packed_size(chunk, channels)
    cond_size = packed_size(cols, channels)
    act_size = packed_size(per_row * group, channels)
    att_size = frames_dev * (channels // 128) + frames_dev // 2
    encoding = jnp.asarray(positions(frames, channels))
    square = (channels, channels)
    dma = pltpu.SemaphoreType.DMA
    values = [
        latents.reshape(frames_dev, n, pix, channels),
        condition,
        key_frames,
        propagate,
        encoding,
        attention_gain,
        conv_gain,
        encoder_conv,
        zero_conv,
        query_weight,
        key_weight,
        value_weight,
        output_weight,
        block_conv,
    ]
    values = [pltpu.with_memory_space_constraint(v, pltpu.MemorySpace.HBM) for v in values]
    return pl.pallas_call(
        functools.partial(kernel, n, row_total),
        out_shape=pltpu.VMEM(latents.shape, BF16),
        in_specs=[pl.BlockSpec(memory_space=pl.ANY)] * len(values),
        out_specs=pl.BlockSpec(memory_space=pltpu.VMEM),
        scratch_shapes=[
            pltpu.SMEM(key_frames.shape, jnp.int32),
            pltpu.SMEM(propagate.shape, jnp.int32),
            pltpu.VMEM((frames, channels), F32),
            pltpu.VMEM((channels,), F32),
            pltpu.VMEM((channels,), F32),
            pltpu.VMEM(condition.shape, BF16),
            pltpu.VMEM((3, channels, wide), BF16),
            pltpu.VMEM((9, channels, tail), BF16),
            pltpu.VMEM(square, BF16),
            pltpu.VMEM(square, BF16),
            pltpu.VMEM(square, BF16),
            pltpu.VMEM(square, BF16),
            pltpu.VMEM(square, BF16),
            pltpu.VMEM((3, channels, wide), BF16),
            pltpu.VMEM((9, channels, tail), BF16),
            pltpu.VMEM(square, BF16),
            pltpu.VMEM((channels, 64 * HEADS), BF16),
            pltpu.VMEM((channels, 64 * HEADS), BF16),
            pltpu.VMEM((2, HEADS // 2, 2 * block, 128), BF16),
            pltpu.VMEM((2, block, 64 * HEADS), BF16),
            pltpu.VMEM((2, channels, block), BF16),
            pltpu.VMEM((2, block, 2 * block), F32),
            pltpu.VMEM((2, block, 2 * block), BF16),
            pltpu.VMEM((channels, block), F32),
            pltpu.VMEM((frames_dev, n, pix, channels), BF16),
            pltpu.VMEM((n, frames_dev, lat_size, 128), BF16),
            pltpu.VMEM((frames, lat_size, 128), BF16),
            pltpu.VMEM((n, chunks, slots, res_size, 128), BF16),
            [pltpu.VMEM((slots * n, res_size, 128), BF16) for _ in range(chunks)],
            pltpu.VMEM((frames, pix, channels), F32),
            pltpu.VMEM((pieces, n, att_size, group, 128), BF16),
            pltpu.VMEM((n, pieces, att_size, group, 128), BF16),
            pltpu.VMEM((frames_dev, n, pieces, group, channels), BF16),
            pltpu.VMEM((frames_dev, rows, per_row, pieces, group, channels), BF16),
            pltpu.VMEM((2, slots, cond_size, 128), BF16),
            pltpu.VMEM((slots, cond_size, 128), BF16),
            pltpu.VMEM((slots, cond_size, 128), BF16),
            pltpu.VMEM((2, pieces, frames_dev, act_size, 128), BF16),
            pltpu.VMEM((pieces, frames_dev, act_size, 128), BF16),
            pltpu.VMEM((pieces, frames_dev, act_size, 128), BF16),
            pltpu.VMEM((slots, rows, cols, wide), F32),
            pltpu.VMEM((frames_dev, rows, per_row, pieces, group, wide), F32),
            dma((16,)),
            dma((7,)),
            dma((1,)),
            dma((chunks,)),
            dma((pieces,)),
            dma((2,)),
            dma((2, pieces)),
        ],
        compiler_params=pltpu.CompilerParams(
            collective_id=0, has_side_effects=True, vmem_limit_bytes=48 * 1024 * 1024
        ),
    )(*values)


def solution(mesh):
    placed = (
        P(("group", "frame"), "row", None, None),
        P(("group", "frame"), "row", None, None),
        P("group"),
        P("group"),
        P(),
        P(),
        P(),
        P(),
        P(),
        P(),
        P(),
        P(),
        P(),
    )
    return jax.shard_map(
        shards,
        mesh=mesh,
        in_specs=placed,
        out_specs=P(("group", "frame"), "row", None, None),
        check_vma=False,
    )
```

```python
import functools
import math

import jax
import jax.numpy as jnp
import numpy as np
from jax import lax
from jax.experimental import pallas as pl
from jax.experimental.pallas import tpu as pltpu
from jax.sharding import PartitionSpec as P

HEADS = 8
MESH = pl.DeviceIdType.MESH
F32 = jnp.float32
BF16 = jnp.bfloat16


def positions(frame_total, channels):
    frame_pos = np.arange(frame_total, dtype=np.float64)[:, None]
    half_index = np.arange(channels // 2, dtype=np.float64)
    frequency = np.exp(half_index * (-2.0 * math.log(10000.0) / channels))
    angles = frame_pos * frequency
    stacked = np.stack([np.sin(angles), np.cos(angles)], axis=-1)
    return stacked.reshape(frame_total, channels).astype(np.float32)


def norm(values, gain):
    average = jnp.mean(values, axis=-1, keepdims=True)
    centered = values - average
    variance = jnp.mean(centered * centered, axis=-1, keepdims=True)
    return centered * lax.rsqrt(variance + 1e-05) * gain


def silu(values):
    half = 0.5 * values
    return half + half * jnp.tanh(half)


def dot(left, right):
    return jnp.dot(left, right, preferred_element_type=F32)


def dot_nt(left, right):
    return lax.dot_general(left, right, (((1,), (1,)), ((), ())), preferred_element_type=F32)


def flat(values):
    return values.astype(F32).reshape(-1, values.shape[-1]).astype(BF16)


def pack_rows(values):
    size = values.shape[1]
    whole = values.shape[2] // 128 * 128
    parts = [values[:, :, low : low + 128] for low in range(0, whole, 128)]
    tail = values[:, :, whole:]
    if size % 16 == 0:
        parts.append(jnp.concatenate([tail[:, : size // 2], tail[:, size // 2 :]], axis=2))
    else:
        parts.append(jnp.concatenate([tail, jnp.zeros_like(tail)], axis=2))
    return jnp.concatenate(parts, axis=1)


def packed_size(size, channels):
    return size * (channels // 128) + (size // 2 if size % 16 == 0 else size)


def unpack_rows(ref, index, size, channels, low, count):
    whole = channels // 128
    rest = channels - whole * 128
    def take(start, rows):
        if isinstance(index, tuple):
            return ref[index[0], :, start : start + rows].astype(F32)
        return ref[index, start : start + rows].astype(F32)

    parts = [take(i * size + low, count) for i in range(whole)]
    if size % 16:
        tail = take(whole * size + low, count)[..., :rest]
    else:
        half = size // 2
        start = low % half
        tile = take(whole * size + start, min(count, half))
        if count == size:
            tail = jnp.concatenate([tile[..., :rest], tile[..., rest:]], axis=-2)
        else:
            tail = tile[..., :rest] if low < half else tile[..., rest:]
    return jnp.concatenate(parts + [tail], axis=-1)


def pack_lead(values):
    count = values.shape[0]
    whole = values.shape[2] // 128 * 128
    parts = [values[:, :, low : low + 128] for low in range(0, whole, 128)]
    tail = values[:, :, whole:]
    parts.append(jnp.concatenate([tail[: count // 2], tail[count // 2 :]], axis=2))
    return jnp.concatenate(parts, axis=0)


def unpack_lead(values, count, channels):
    whole = channels // 128
    rest = channels - whole * 128
    parts = [values[i * count : (i + 1) * count] for i in range(whole)]
    tile = values[whole * count :]
    parts.append(jnp.concatenate([tile[..., :rest], tile[..., rest:]], axis=0))
    return jnp.concatenate(parts, axis=-1)


def pack_tails(tails, packed, main):
    wide = 3 * main
    for a in range(3):
        parts = [tails[3 * a + b] for b in range(3)]
        packed[a, :, wide:] = jnp.concatenate(parts, axis=1)


def conv_local(images, packed, put, add):
    rows = images.shape[1]
    put(slice(0, rows), dot(flat(images), packed[1]))
    if rows > 1:
        add(slice(1, rows), dot(flat(images[:, : rows - 1]), packed[0]))
        add(slice(0, rows - 1), dot(flat(images[:, 1:]), packed[2]))


def pair_tiles(weight, width):
    rows, channels = weight.shape
    tiles = []
    for low in range(0, channels, width):
        tiles.append(weight[:, low : low + width])
        tiles.append(jnp.zeros((rows, 128 - width), weight.dtype))
    return jnp.concatenate(tiles, axis=1)


def conv_row(total, main, tail):
    cols = total.shape[0]
    col = lax.broadcasted_iota(jnp.int32, (cols, 1), 0)
    pieces = []
    for start, size in ((0, main), (3 * main, tail)):
        left, middle, right = (total[:, start + b * size : start + (b + 1) * size] for b in range(3))
        left = jnp.where(col == 0, 0.0, pltpu.roll(left, 1, 0))
        right = jnp.where(col == cols - 1, 0.0, pltpu.roll(right, cols - 1, 0))
        pieces.append(left + middle + right)
    return jnp.concatenate(pieces, axis=1)


def kernel(
    n,
    row_total,
    lat,
    cond_hbm,
    key_hbm,
    prop_hbm,
    encoding_hbm,
    gain_a_hbm,
    gain_c_hbm,
    enc_hbm,
    zero_hbm,
    q_hbm,
    k_hbm,
    v_hbm,
    o_hbm,
    blk_hbm,
    sums_b,
    att,
    key_frames,
    propagate,
    encoding,
    gain_a,
    gain_c,
    cond,
    enc_w,
    enc_t,
    squares,
    blk_w,
    blk_t,
    v_wt,
    q_wp,
    k_wp,
    normed,
    q_both,
    k_held,
    v_held,
    scores,
    probs,
    mixed_t,
    lat_own,
    lat_out,
    lat_pix,
    res_out,
    res_pix,
    hidden,
    att_out,
    att_in,
    act,
    cond_out,
    cond_top,
    cond_bot,
    act_out,
    act_top,
    act_bot,
    sums_e,
    w_sem,
    send,
    lat_recv,
    res_recv,
    att_recv,
    ch_recv,
    ah_recv,
):
    me = lax.axis_index("frame")
    row_me = lax.axis_index("row")
    frames_dev, _, pix, channels = lat.shape
    slots, rows, cols, _ = cond.shape
    chunks = res_recv.shape[0]
    chunk = pix // chunks
    frames = hidden.shape[0]
    pieces, group = att.shape[2:4]
    per_chunk = chunk // group
    per_row = n // rows
    head_dim = channels // HEADS
    main = enc_w.shape[2] // 3 // 128 * 128
    tail = channels - main
    has_up = row_me > 0
    has_down = row_me < row_total - 1

    barrier = pltpu.get_barrier_semaphore()
    for k in range(1, n):
        pl.semaphore_signal(
            barrier, inc=1, device_id={"frame": lax.rem(me + k, n)}, device_id_type=MESH
        )

    @pl.when(has_up)
    def _():
        pl.semaphore_signal(barrier, inc=1, device_id={"row": row_me - 1}, device_id_type=MESH)

    @pl.when(has_down)
    def _():
        pl.semaphore_signal(barrier, inc=1, device_id={"row": row_me + 1}, device_id_type=MESH)

    def start_taps(src, packed, sem):
        for a in range(3):
            for b in range(3):
                pltpu.make_async_copy(
                    src.at[3 * a + b, :, :main], packed.at[a, :, b * main : (b + 1) * main], sem
                ).start()

    def wait_taps(packed, sem):
        whole = packed.at[:, :, : 3 * main]
        pltpu.make_async_copy(whole, whole, sem).wait()

    pairs = [
        (cond_hbm, cond),
        (lat, lat_own),
        (enc_hbm.at[:, :, main:], enc_t),
        (blk_hbm.at[:, :, main:], blk_t),
        (encoding_hbm, encoding),
        (gain_a_hbm, gain_a),
        (gain_c_hbm, gain_c),
        (key_hbm, key_frames),
        (prop_hbm, propagate),
    ]
    loads = [pltpu.make_async_copy(s, d, w_sem.at[3 + i]) for i, (s, d) in enumerate(pairs)]
    loads[0].start()
    loads[1].start()
    loads[2].start()

    @pl.when(jnp.logical_not(has_up))
    def _():
        cond_top[...] = jnp.zeros_like(cond_top)
        act_top[...] = jnp.zeros_like(act_top)

    @pl.when(jnp.logical_not(has_down))
    def _():
        cond_bot[...] = jnp.zeros_like(cond_bot)
        act_bot[...] = jnp.zeros_like(act_bot)

    start_taps(enc_hbm, enc_w, w_sem.at[0])
    loads[0].wait()
    cond_out[0] = pack_rows(cond[:, 0].astype(F32)).astype(BF16)
    cond_out[1] = pack_rows(cond[:, rows - 1].astype(F32)).astype(BF16)
    neighbours = has_up.astype(jnp.int32) + has_down.astype(jnp.int32)
    with jax.named_scope("w_barrier"):
        pl.semaphore_wait(barrier, n - 1 + neighbours)

    def remote(src, dst, send_sem, recv_sem, **where):
        return pltpu.make_async_remote_copy(
            src_ref=src,
            dst_ref=dst,
            send_sem=send_sem,
            recv_sem=recv_sem,
            device_id=where,
            device_id_type=MESH,
        )

    def up(src, dst, send_sem, recv_sem):
        return remote(src, dst, send_sem, recv_sem, row=row_me - 1)

    def down(src, dst, send_sem, recv_sem):
        return remote(src, dst, send_sem, recv_sem, row=row_me + 1)

    def drain(ref, sem):
        pltpu.make_async_copy(ref, ref, sem).wait()

    cond_up = up(cond_out.at[0], cond_bot, send.at[0], ch_recv.at[0])
    cond_down = down(cond_out.at[1], cond_top, send.at[1], ch_recv.at[1])
    pl.when(has_up)(cond_up.start)
    pl.when(has_down)(cond_down.start)

    loads[1].wait()
    for p in range(n):
        lat_out[p] = pack_rows(lat_own[:, p].astype(F32)).astype(BF16)
    peers = [lax.rem(me + k, n) for k in range(1, n)]
    for peer in peers:
        remote(
            lat_out.at[peer],
            lat_pix.at[pl.ds(me * frames_dev, frames_dev)],
            send.at[2],
            lat_recv.at[0],
            frame=peer,
        ).start()
    lat_pix[pl.ds(me * frames_dev, frames_dev)] = lat_out[me]
    for i, source in enumerate((v_hbm, zero_hbm, q_hbm, k_hbm, o_hbm)):
        pltpu.make_async_copy(source, squares.at[i], w_sem.at[2]).start()
    for load in loads[3:]:
        load.start()
    start_taps(blk_hbm, blk_w, w_sem.at[1])

    with jax.named_scope("w_load01"):
        loads[2].wait()
    with jax.named_scope("pack_enc"):
        pack_tails(enc_t, enc_w, main)
        wait_taps(enc_w, w_sem.at[0])

    def edge_rows(ref, index, size):
        values = unpack_rows(ref, index, size, channels, 0, size)
        return values.reshape(-1, channels).astype(BF16)

    def put_e(r, value):
        sums_e[:, r] = value.reshape(slots, -1, cols, value.shape[-1])

    def add_e(r, value):
        sums_e[:, r] += value.reshape(slots, -1, cols, value.shape[-1])

    with jax.named_scope("encconv_local"):
        conv_local(cond[...], enc_w, put_e, add_e)
    with jax.named_scope("prep"):
        drain(squares, w_sem.at[2])
        v_wt[...] = jnp.transpose(squares[0].astype(F32)).astype(BF16)
        q_wp[...] = pair_tiles(squares[2], 2 * head_dim)
        k_wp[...] = pair_tiles(squares[3], 2 * head_dim)
        loads[3].wait()
        pack_tails(blk_t, blk_w, main)
    with jax.named_scope("w_condhalo"):
        pl.when(has_up)(cond_down.wait_recv)
        pl.when(has_down)(cond_up.wait_recv)
    with jax.named_scope("encconv_edge"):
        add_e(slice(0, 1), dot(edge_rows(cond_top, slice(None), cols), enc_w[0]))
        add_e(slice(rows - 1, rows), dot(edge_rows(cond_bot, slice(None), cols), enc_w[2]))
    with jax.named_scope("enc_silu_zero"):
        encoded = jnp.concatenate(
            [silu(conv_row(sums_e[s, r], main, tail)) for s in range(slots) for r in range(rows)],
            axis=0,
        ).astype(BF16)
        keyres = dot(encoded, squares[1]).reshape(slots, n, pix, channels)
        for p in range(n):
            for c in range(chunks):
                part = pack_rows(keyres[:, p, c * chunk : (c + 1) * chunk])
                res_out[p, c] = part.astype(BF16)
    for c in range(chunks):
        for peer in peers:
            remote(
                res_out.at[peer, c],
                res_pix[c].at[pl.ds(me * slots, slots)],
                send.at[3],
                res_recv.at[c],
                frame=peer,
            ).start()
    for c in range(chunks):
        res_pix[c][pl.ds(me * slots, slots)] = res_out[me, c]

    with jax.named_scope("w_loads"):
        for load in loads[4:]:
            load.wait()
    with jax.named_scope("w_lat"):
        drain(lat_pix.at[: (n - 1) * frames_dev], lat_recv.at[0])

    small = frames <= 24
    block = frames * group
    factor = math.log2(math.e) / math.sqrt(head_dim)
    encode = encoding[...][:, None, :]
    lane = lax.broadcasted_iota(jnp.int32, (1, 128), 1)
    pairs_total = HEADS // 2

    def soft(values):
        width = values.shape[-1]
        values = values.reshape(frames, group, width)
        top = jnp.max(values, axis=0, keepdims=True)
        powers = jnp.exp2(values - top)
        total = jnp.sum(powers, axis=0, keepdims=True)
        pixel = lax.broadcasted_iota(jnp.int32, (1, group, width), 1)
        query = lax.broadcasted_iota(jnp.int32, (1, group, width), 2)
        weight = jnp.where(lax.rem(query, group) == pixel, 1.0 / total, 0.0)
        return (powers * weight).reshape(block, width).astype(BF16)

    def hide(c):
        span = slice(c * chunk, (c + 1) * chunk)
        drain(res_pix[c].at[: (n - 1) * slots], res_recv.at[c])

        def one(f, carry):
            slot = propagate[f]
            gap = jnp.abs(f - key_frames[slot]).astype(F32)
            reach = jnp.exp(jnp.full((1, channels), -gap / (2 * frames_dev), F32))
            residual = unpack_rows(res_pix[c], slot, chunk, channels, 0, chunk)
            value = unpack_rows(lat_pix, f, pix, channels, c * chunk, chunk) + reach * residual
            hidden[f, span] = value
            return carry

        lax.fori_loop(0, frames, one, 0, unroll=small)

    mask = jnp.where(lane < head_dim, 1.0, 0.0).astype(BF16)
    other = jnp.where(lane < head_dim, 0.0, 1.0).astype(BF16)

    def prepare(s):
        base = hidden[:, s * group : (s + 1) * group]
        value = norm(base, gain_a[...]) + encode
        normed[s % 2] = value.reshape(block, channels).astype(BF16)

    def project_q(s, t):
        query = dot(normed[s % 2], q_wp[:, 256 * t : 256 * (t + 1)]) * factor
        query = query.astype(BF16)
        for i in range(2):
            tile = query[:, 128 * i : 128 * (i + 1)]
            q_both[s % 2, 2 * t + i, :block] = tile * mask
            q_both[s % 2, 2 * t + i, block:] = tile * other

    def project_k(s, t):
        keys = dot(normed[s % 2], k_wp[:, 256 * t : 256 * (t + 1)])
        k_held[s % 2, :, 256 * t : 256 * (t + 1)] = keys.astype(BF16)

    def project_v(s):
        v_held[s % 2] = dot_nt(v_wt[...], normed[s % 2]).astype(BF16)

    def project(s):
        prepare(s)
        for t in range(pairs_total // 2):
            project_q(s, t)
            project_k(s, t)
        project_v(s)

    def score(s, j):
        keys = k_held[s % 2, :, 128 * j : 128 * (j + 1)]
        scores[j % 2] = dot_nt(keys, q_both[s % 2, j])

    def soften(s, j, low, high):
        probs[j % 2, :, low:high] = soft(scores[j % 2, :, low:high])

    def mix(s, j):
        low, high = 2 * j * head_dim, 2 * (j + 1) * head_dim
        pair = dot(v_held[s % 2, low:high], probs[j % 2])
        mixed_t[low : low + head_dim] = pair[:head_dim, :block]
        mixed_t[low + head_dim : high] = pair[head_dim:, block:]

    def finish(s):
        mixed = jnp.transpose(mixed_t[...]).astype(BF16)
        projected = dot(mixed, squares[4]).reshape(frames, group, channels)
        base = hidden[:, s * group : (s + 1) * group]
        total = base + projected
        for p in range(n):
            part = pack_lead(total[p * frames_dev : (p + 1) * frames_dev])
            att_out[s, p] = part.astype(BF16)
        for peer in peers:
            remote(
                att_out.at[s, peer],
                att_in.at[me, s],
                send.at[4],
                att_recv.at[s],
                frame=peer,
            ).start()
        att_in[me, s] = att_out[s, me]

    def activate(s):
        with jax.named_scope(f"w_att{s}"):
            drain(att_in.at[: n - 1, s], att_recv.at[s])
        with jax.named_scope(f"act{s}"):
            taken = [unpack_lead(att_in[p, s].astype(F32), frames_dev, channels) for p in range(n)]
            value = jnp.stack(taken, axis=1)
            att[:, :, s] = value.astype(BF16)
            value = silu(norm(value, gain_c[...])).reshape(frames_dev, rows, -1, channels)
            act_out[0, s] = pack_rows(value[:, 0]).astype(BF16)
            act_out[1, s] = pack_rows(value[:, rows - 1]).astype(BF16)
            value = value.reshape(frames_dev, rows, per_row, group, channels)
            act[:, :, :, s] = value.astype(BF16)
        which = 1 if s == pieces - 1 else 0
        act_up = up(act_out.at[0, s], act_bot.at[s], send.at[5], ah_recv.at[0, which])
        act_down = down(act_out.at[1, s], act_top.at[s], send.at[6], ah_recv.at[1, which])
        pl.when(has_up)(act_up.start)
        pl.when(has_down)(act_down.start)

    def attend_all():
        turns = [(s, j) for s in range(pieces) for j in range(pairs_total)]
        tiles = [(low, min(low + 128, 2 * block)) for low in range(0, 2 * block, 128)]
        hide(0)
        project(0)
        score(0, 0)
        for k, (s, j) in enumerate(turns):
            work = []
            if k > 0:
                work.append(functools.partial(mix, *turns[k - 1]))
            if k + 1 < len(turns) and j + 1 < pairs_total:
                work.append(functools.partial(score, s, j + 1))
            if j == 0 and s > 0:
                work.append(functools.partial(finish, s - 1))
            if s + 1 < pieces:
                if j == 1:
                    if (s + 1) % per_chunk == 0:
                        hide((s + 1) // per_chunk)
                    work.append(functools.partial(prepare, s + 1))
                    work.append(functools.partial(project_q, s + 1, 0))
                if j == 2:
                    work.append(functools.partial(project_q, s + 1, 1))
                    work.append(functools.partial(project_k, s + 1, 0))
                if j == 3:
                    work.append(functools.partial(project_k, s + 1, 1))
                    work.append(functools.partial(project_v, s + 1))
                    work.append(functools.partial(score, s + 1, 0))
            for i in range(max(len(tiles), len(work))):
                if i < len(tiles):
                    soften(s, j, *tiles[i])
                if i < len(work):
                    work[i]()
            if (pieces - s, j) == (1, 3) and pieces > 1:
                activate(0)
        mix(*turns[-1])
        finish(pieces - 1)

    with jax.named_scope("attention"):
        if small:
            attend_all()
        else:
            for s in range(pieces):
                if s % per_chunk == 0:
                    hide(s // per_chunk)
                project(s)

                def step(j, carry):
                    keys = k_held[s % 2, :, pl.ds(pl.multiple_of(128 * j, 128), 128)]
                    for i in range(2):
                        part = q_both[s % 2, j, i * block : (i + 1) * block]
                        row = pl.ds(pl.multiple_of((2 * j + i) * head_dim, 8), head_dim)
                        value = dot(v_held[s % 2], soft(dot_nt(keys, part)))
                        scores[0, :channels, :block] = value
                        mixed_t[row] = scores[0, row, :block]
                    return carry

                lax.fori_loop(0, pairs_total, step, 0)
                finish(s)

    def add_b(r, span, ref, taps):
        parts = [edge_rows(ref, (s,), per_row * group) for s in range(span.start, span.stop)]
        value = dot(jnp.concatenate(parts, axis=0), taps)
        value = value.reshape(len(parts), frames_dev, per_row, group, value.shape[-1])
        for i, s in enumerate(range(span.start, span.stop)):
            sums_b[:, r, :, s] += value[i]

    def put_all(r, value):
        sums_b[:, r] = value.reshape(frames_dev, -1, per_row, pieces, group, value.shape[-1])

    def add_all(r, value):
        sums_b[:, r] += value.reshape(frames_dev, -1, per_row, pieces, group, value.shape[-1])

    early = 1 if small and pieces > 1 else 0
    for s in range(early, pieces):
        activate(s)
    wait_taps(blk_w, w_sem.at[1])
    with jax.named_scope("blkconv_local"):
        conv_local(act[...].reshape(frames_dev, rows, -1, group, channels), blk_w, put_all, add_all)
    last = max(pieces - 1, 0)
    for span in [slice(0, last), slice(last, pieces)] if last else [slice(0, pieces)]:
        with jax.named_scope(f"w_acthalo{span.start}"):
            which = 1 if span.stop == pieces else 0
            pl.when(has_up)(lambda: drain(act_top.at[span], ah_recv.at[1, which]))
            pl.when(has_down)(lambda: drain(act_bot.at[span], ah_recv.at[0, which]))
        with jax.named_scope(f"blkconv_edge{span.start}"):
            add_b(0, span, act_top, blk_w[0])
            add_b(rows - 1, span, act_bot, blk_w[2])
    with jax.named_scope("w_end"):
        pl.when(has_up)(cond_up.wait_send)
        pl.when(has_down)(cond_down.wait_send)
        drain(lat_pix.at[: (n - 1) * frames_dev], send.at[2])
        drain(res_out.at[: n - 1], send.at[3])
        drain(att_out.at[:, : n - 1], send.at[4])
        pl.when(has_up)(lambda: drain(act_out.at[0], send.at[5]))
        pl.when(has_down)(lambda: drain(act_out.at[1], send.at[6]))


def add_up(main, tail, sums, att, out_hbm, out, sem):
    frames_dev, rows, cols, channels = out.shape
    per_row = sums.shape[2]
    stores = []
    for f in range(frames_dev):
        for r in range(rows):
            convolved = conv_row(sums[f, r].reshape(cols, -1), main, tail)
            held = att[f, r * per_row : (r + 1) * per_row].astype(F32).reshape(cols, channels)
            out[f, r] = (held + convolved).astype(BF16)
        stores.append(pltpu.make_async_copy(out.at[f], out_hbm.at[f], sem.at[f]))
        stores[f].start()
    for store in stores:
        store.wait()


def shards(
    latents,
    condition,
    key_frames,
    propagate,
    encoder_conv,
    zero_conv,
    attention_gain,
    query_weight,
    key_weight,
    value_weight,
    output_weight,
    conv_gain,
    block_conv,
):
    frames_dev, rows, cols, channels = latents.shape
    slots = condition.shape[0]
    n = lax.axis_size("frame")
    row_total = lax.axis_size("row")
    pix = rows * cols // n
    frames = frames_dev * n
    chunk = 16 if pix % 16 == 0 else 8
    chunks = pix // chunk
    group = 8
    pieces = pix // group
    block = frames * group
    per_row = n // rows
    main = channels // 256 * 256
    tail = channels - main
    wide = 3 * (main + tail)
    lat_size = packed_size(pix, channels)
    res_size = packed_size(chunk, channels)
    cond_size = packed_size(cols, channels)
    act_size = packed_size(per_row * group, channels)
    att_size = frames_dev * (channels // 128) + frames_dev // 2
    encoding = jnp.asarray(positions(frames, channels))
    square = (channels, channels)
    dma = pltpu.SemaphoreType.DMA
    values = [
        latents.reshape(frames_dev, n, pix, channels),
        condition,
        key_frames,
        propagate,
        encoding,
        attention_gain,
        conv_gain,
        encoder_conv,
        zero_conv,
        query_weight,
        key_weight,
        value_weight,
        output_weight,
        block_conv,
    ]
    values = [pltpu.with_memory_space_constraint(v, pltpu.MemorySpace.HBM) for v in values]
    sums_shape = pltpu.VMEM((frames_dev, rows, per_row, pieces, group, wide), F32)
    att_shape = pltpu.VMEM((frames_dev, n, pieces, group, channels), BF16)
    vmem = pl.BlockSpec(memory_space=pltpu.VMEM)
    sums, att = pl.pallas_call(
        functools.partial(kernel, n, row_total),
        out_shape=(sums_shape, att_shape),
        in_specs=[pl.BlockSpec(memory_space=pl.ANY)] * len(values),
        out_specs=(vmem, vmem),
        scratch_shapes=[
            pltpu.SMEM(key_frames.shape, jnp.int32),
            pltpu.SMEM(propagate.shape, jnp.int32),
            pltpu.VMEM((frames, channels), F32),
            pltpu.VMEM((channels,), F32),
            pltpu.VMEM((channels,), F32),
            pltpu.VMEM(condition.shape, BF16),
            pltpu.VMEM((3, channels, wide), BF16),
            pltpu.VMEM((9, channels, tail), BF16),
            pltpu.VMEM((5,) + square, BF16),
            pltpu.VMEM((3, channels, wide), BF16),
            pltpu.VMEM((9, channels, tail), BF16),
            pltpu.VMEM(square, BF16),
            pltpu.VMEM((channels, 64 * HEADS), BF16),
            pltpu.VMEM((channels, 64 * HEADS), BF16),
            pltpu.VMEM((2, block, channels), BF16),
            pltpu.VMEM((2, HEADS // 2, 2 * block, 128), BF16),
            pltpu.VMEM((2, block, 64 * HEADS), BF16),
            pltpu.VMEM((2, channels, block), BF16),
            pltpu.VMEM((2, block, 2 * block), F32),
            pltpu.VMEM((2, block, 2 * block), BF16),
            pltpu.VMEM((channels, block), F32),
            pltpu.VMEM((frames_dev, n, pix, channels), BF16),
            pltpu.VMEM((n, frames_dev, lat_size, 128), BF16),
            pltpu.VMEM((frames, lat_size, 128), BF16),
            pltpu.VMEM((n, chunks, slots, res_size, 128), BF16),
            [pltpu.VMEM((slots * n, res_size, 128), BF16) for _ in range(chunks)],
            pltpu.VMEM((frames, pix, channels), F32),
            pltpu.VMEM((pieces, n, att_size, group, 128), BF16),
            pltpu.VMEM((n, pieces, att_size, group, 128), BF16),
            pltpu.VMEM((frames_dev, rows, per_row, pieces, group, channels), BF16),
            pltpu.VMEM((2, slots, cond_size, 128), BF16),
            pltpu.VMEM((slots, cond_size, 128), BF16),
            pltpu.VMEM((slots, cond_size, 128), BF16),
            pltpu.VMEM((2, pieces, frames_dev, act_size, 128), BF16),
            pltpu.VMEM((pieces, frames_dev, act_size, 128), BF16),
            pltpu.VMEM((pieces, frames_dev, act_size, 128), BF16),
            pltpu.VMEM((slots, rows, cols, wide), F32),
            dma((12,)),
            dma((7,)),
            dma((1,)),
            dma((chunks,)),
            dma((pieces,)),
            dma((2,)),
            dma((2, 2)),
        ],
        compiler_params=pltpu.CompilerParams(
            collective_id=0, has_side_effects=True, vmem_limit_bytes=48 * 1024 * 1024
        ),
    )(*values)
    return pl.pallas_call(
        functools.partial(add_up, main, tail),
        out_shape=jax.ShapeDtypeStruct(latents.shape, BF16),
        in_specs=[vmem, vmem],
        out_specs=pl.BlockSpec(memory_space=pl.ANY),
        scratch_shapes=[pltpu.VMEM(latents.shape, BF16), dma((frames_dev,))],
        compiler_params=pltpu.CompilerParams(vmem_limit_bytes=4 * 1024 * 1024),
    )(sums, att)


def solution(mesh):
    placed = (
        P(("group", "frame"), "row", None, None),
        P(("group", "frame"), "row", None, None),
        P("group"),
        P("group"),
        P(),
        P(),
        P(),
        P(),
        P(),
        P(),
        P(),
        P(),
        P(),
    )
    return jax.shard_map(
        shards,
        mesh=mesh,
        in_specs=placed,
        out_specs=P(("group", "frame"), "row", None, None),
        check_vma=False,
    )
```

```python
import functools
import math

import jax
import jax.numpy as jnp
import numpy as np
from jax import lax
from jax.experimental import pallas as pl
from jax.experimental.pallas import tpu as pltpu
from jax.sharding import PartitionSpec as P

HEADS = 8
MESH = pl.DeviceIdType.MESH
F32 = jnp.float32
BF16 = jnp.bfloat16


def positions(frame_total, channels):
    frame_pos = np.arange(frame_total, dtype=np.float64)[:, None]
    half_index = np.arange(channels // 2, dtype=np.float64)
    frequency = np.exp(half_index * (-2.0 * math.log(10000.0) / channels))
    angles = frame_pos * frequency
    stacked = np.stack([np.sin(angles), np.cos(angles)], axis=-1)
    return stacked.reshape(frame_total, channels).astype(np.float32)


def norm(values, gain):
    average = jnp.mean(values, axis=-1, keepdims=True)
    centered = values - average
    variance = jnp.mean(centered * centered, axis=-1, keepdims=True)
    return centered * lax.rsqrt(variance + 1e-05) * gain


def silu(values):
    half = 0.5 * values
    return half + half * jnp.tanh(half)


def dot(left, right):
    return jnp.dot(left, right, preferred_element_type=F32)


def dot_nt(left, right):
    return lax.dot_general(left, right, (((1,), (1,)), ((), ())), preferred_element_type=F32)


def flat(values):
    return values.astype(F32).reshape(-1, values.shape[-1]).astype(BF16)


def pack_rows(values):
    size = values.shape[1]
    whole = values.shape[2] // 128 * 128
    parts = [values[:, :, low : low + 128] for low in range(0, whole, 128)]
    tail = values[:, :, whole:]
    if size % 16 == 0:
        parts.append(jnp.concatenate([tail[:, : size // 2], tail[:, size // 2 :]], axis=2))
    else:
        parts.append(jnp.concatenate([tail, jnp.zeros_like(tail)], axis=2))
    return jnp.concatenate(parts, axis=1)


def packed_size(size, channels):
    return size * (channels // 128) + (size // 2 if size % 16 == 0 else size)


def unpack_rows(ref, index, size, channels, low, count):
    whole = channels // 128
    rest = channels - whole * 128
    def take(start, rows):
        if isinstance(index, tuple):
            return ref[index[0], :, start : start + rows].astype(F32)
        return ref[index, start : start + rows].astype(F32)

    parts = [take(i * size + low, count) for i in range(whole)]
    if size % 16:
        tail = take(whole * size + low, count)[..., :rest]
    else:
        half = size // 2
        start = low % half
        tile = take(whole * size + start, min(count, half))
        if count == size:
            tail = jnp.concatenate([tile[..., :rest], tile[..., rest:]], axis=-2)
        else:
            tail = tile[..., :rest] if low < half else tile[..., rest:]
    return jnp.concatenate(parts + [tail], axis=-1)


def pack_lead(values):
    count = values.shape[0]
    whole = values.shape[2] // 128 * 128
    parts = [values[:, :, low : low + 128] for low in range(0, whole, 128)]
    tail = values[:, :, whole:]
    parts.append(jnp.concatenate([tail[: count // 2], tail[count // 2 :]], axis=2))
    return jnp.concatenate(parts, axis=0)


def unpack_lead(values, count, channels):
    whole = channels // 128
    rest = channels - whole * 128
    parts = [values[i * count : (i + 1) * count] for i in range(whole)]
    tile = values[whole * count :]
    parts.append(jnp.concatenate([tile[..., :rest], tile[..., rest:]], axis=0))
    return jnp.concatenate(parts, axis=-1)


def pack_tails(tails, packed, main):
    wide = 3 * main
    for a in range(3):
        parts = [tails[3 * a + b] for b in range(3)]
        packed[a, :, wide:] = jnp.concatenate(parts, axis=1)


def conv_local(images, packed, put, add):
    rows = images.shape[1]
    put(slice(0, rows), dot(flat(images), packed[1]))
    if rows > 1:
        add(slice(1, rows), dot(flat(images[:, : rows - 1]), packed[0]))
        add(slice(0, rows - 1), dot(flat(images[:, 1:]), packed[2]))


def pair_tiles(weight, width):
    rows, channels = weight.shape
    tiles = []
    for low in range(0, channels, width):
        tiles.append(weight[:, low : low + width])
        tiles.append(jnp.zeros((rows, 128 - width), weight.dtype))
    return jnp.concatenate(tiles, axis=1)


def conv_row(total, main, tail):
    cols = total.shape[0]
    col = lax.broadcasted_iota(jnp.int32, (cols, 1), 0)
    pieces = []
    for start, size in ((0, main), (3 * main, tail)):
        left, middle, right = (total[:, start + b * size : start + (b + 1) * size] for b in range(3))
        left = jnp.where(col == 0, 0.0, pltpu.roll(left, 1, 0))
        right = jnp.where(col == cols - 1, 0.0, pltpu.roll(right, cols - 1, 0))
        pieces.append(left + middle + right)
    return jnp.concatenate(pieces, axis=1)


def kernel(
    n,
    row_total,
    lat,
    cond_hbm,
    key_hbm,
    prop_hbm,
    encoding_hbm,
    gain_a_hbm,
    gain_c_hbm,
    enc_hbm,
    zero_hbm,
    q_hbm,
    k_hbm,
    v_hbm,
    o_hbm,
    blk_hbm,
    sums_b,
    att,
    key_frames,
    propagate,
    encoding,
    gain_a,
    gain_c,
    cond,
    enc_w,
    enc_t,
    squares,
    blk_w,
    blk_t,
    v_wt,
    q_wp,
    k_wp,
    normed,
    q_both,
    k_held,
    v_held,
    scores,
    probs,
    mixed_t,
    lat_own,
    lat_out,
    lat_pix,
    res_out,
    res_pix,
    hidden,
    att_out,
    att_in,
    act,
    cond_out,
    cond_top,
    cond_bot,
    act_out,
    act_top,
    act_bot,
    sums_e,
    w_sem,
    send,
    lat_recv,
    res_recv,
    att_recv,
    ch_recv,
    ah_recv,
):
    me = lax.axis_index("frame")
    row_me = lax.axis_index("row")
    frames_dev, _, pix, channels = lat.shape
    slots, rows, cols, _ = cond.shape
    chunks = res_recv.shape[0]
    chunk = pix // chunks
    frames = hidden.shape[0]
    pieces, group = att.shape[3:5]
    per_chunk = chunk // group
    per_row = n // rows
    head_dim = channels // HEADS
    main = enc_w.shape[2] // 3 // 128 * 128
    tail = channels - main
    def block_of(p):
        return p % rows * per_row + p // rows

    home = lax.div(me, rows)
    has_up = row_me > 0
    has_down = row_me < row_total - 1

    barrier = pltpu.get_barrier_semaphore()
    for k in range(1, n):
        pl.semaphore_signal(
            barrier, inc=1, device_id={"frame": lax.rem(me + k, n)}, device_id_type=MESH
        )

    @pl.when(has_up)
    def _():
        pl.semaphore_signal(barrier, inc=1, device_id={"row": row_me - 1}, device_id_type=MESH)

    @pl.when(has_down)
    def _():
        pl.semaphore_signal(barrier, inc=1, device_id={"row": row_me + 1}, device_id_type=MESH)

    def start_taps(src, packed, sem):
        for a in range(3):
            for b in range(3):
                pltpu.make_async_copy(
                    src.at[3 * a + b, :, :main], packed.at[a, :, b * main : (b + 1) * main], sem
                ).start()

    def wait_taps(packed, sem):
        whole = packed.at[:, :, : 3 * main]
        pltpu.make_async_copy(whole, whole, sem).wait()

    pairs = [
        (cond_hbm, cond),
        (lat, lat_own),
        (enc_hbm.at[:, :, main:], enc_t),
        (blk_hbm.at[:, :, main:], blk_t),
        (encoding_hbm, encoding),
        (gain_a_hbm, gain_a),
        (gain_c_hbm, gain_c),
        (key_hbm, key_frames),
        (prop_hbm, propagate),
    ]
    loads = [pltpu.make_async_copy(s, d, w_sem.at[3 + i]) for i, (s, d) in enumerate(pairs)]
    loads[0].start()
    loads[1].start()
    loads[2].start()

    @pl.when(jnp.logical_not(has_up))
    def _():
        cond_top[...] = jnp.zeros_like(cond_top)
        act_top[...] = jnp.zeros_like(act_top)

    @pl.when(jnp.logical_not(has_down))
    def _():
        cond_bot[...] = jnp.zeros_like(cond_bot)
        act_bot[...] = jnp.zeros_like(act_bot)

    start_taps(enc_hbm, enc_w, w_sem.at[0])
    loads[0].wait()
    cond_out[0] = pack_rows(cond[:, 0].astype(F32)).astype(BF16)
    cond_out[1] = pack_rows(cond[:, rows - 1].astype(F32)).astype(BF16)
    neighbours = has_up.astype(jnp.int32) + has_down.astype(jnp.int32)
    with jax.named_scope("w_barrier"):
        pl.semaphore_wait(barrier, n - 1 + neighbours)

    def remote(src, dst, send_sem, recv_sem, **where):
        return pltpu.make_async_remote_copy(
            src_ref=src,
            dst_ref=dst,
            send_sem=send_sem,
            recv_sem=recv_sem,
            device_id=where,
            device_id_type=MESH,
        )

    def up(src, dst, send_sem, recv_sem):
        return remote(src, dst, send_sem, recv_sem, row=row_me - 1)

    def down(src, dst, send_sem, recv_sem):
        return remote(src, dst, send_sem, recv_sem, row=row_me + 1)

    def drain(ref, sem):
        pltpu.make_async_copy(ref, ref, sem).wait()

    cond_up = up(cond_out.at[0], cond_bot, send.at[0], ch_recv.at[0])
    cond_down = down(cond_out.at[1], cond_top, send.at[1], ch_recv.at[1])
    pl.when(has_up)(cond_up.start)
    pl.when(has_down)(cond_down.start)

    loads[1].wait()
    for p in range(n):
        lat_out[p] = pack_rows(lat_own[:, block_of(p)].astype(F32)).astype(BF16)
    peers = [lax.rem(me + k, n) for k in range(1, n)]
    for peer in peers:
        remote(
            lat_out.at[peer],
            lat_pix.at[pl.ds(me * frames_dev, frames_dev)],
            send.at[2],
            lat_recv.at[0],
            frame=peer,
        ).start()
    lat_pix[pl.ds(me * frames_dev, frames_dev)] = lat_out[me]
    for i, source in enumerate((v_hbm, zero_hbm, q_hbm, k_hbm, o_hbm)):
        pltpu.make_async_copy(source, squares.at[i], w_sem.at[2]).start()
    for load in loads[3:]:
        load.start()
    start_taps(blk_hbm, blk_w, w_sem.at[1])

    with jax.named_scope("w_load01"):
        loads[2].wait()
    with jax.named_scope("pack_enc"):
        pack_tails(enc_t, enc_w, main)
        wait_taps(enc_w, w_sem.at[0])

    def edge_rows(ref, index, size):
        values = unpack_rows(ref, index, size, channels, 0, size)
        return values.reshape(-1, channels).astype(BF16)

    def put_e(r, value):
        sums_e[:, r] = value.reshape(slots, -1, cols, value.shape[-1])

    def add_e(r, value):
        sums_e[:, r] += value.reshape(slots, -1, cols, value.shape[-1])

    with jax.named_scope("encconv_local"):
        conv_local(cond[...], enc_w, put_e, add_e)
    with jax.named_scope("prep"):
        drain(squares, w_sem.at[2])
        v_wt[...] = jnp.transpose(squares[0].astype(F32)).astype(BF16)
        q_wp[...] = pair_tiles(squares[2], 2 * head_dim)
        k_wp[...] = pair_tiles(squares[3], 2 * head_dim)
        loads[3].wait()
        pack_tails(blk_t, blk_w, main)
    with jax.named_scope("w_condhalo"):
        pl.when(has_up)(cond_down.wait_recv)
        pl.when(has_down)(cond_up.wait_recv)
    with jax.named_scope("encconv_edge"):
        add_e(slice(0, 1), dot(edge_rows(cond_top, slice(None), cols), enc_w[0]))
        add_e(slice(rows - 1, rows), dot(edge_rows(cond_bot, slice(None), cols), enc_w[2]))
    with jax.named_scope("enc_silu_zero"):
        encoded = jnp.concatenate(
            [silu(conv_row(sums_e[s, r], main, tail)) for s in range(slots) for r in range(rows)],
            axis=0,
        ).astype(BF16)
        keyres = dot(encoded, squares[1]).reshape(slots, n, pix, channels)
        for p in range(n):
            for c in range(chunks):
                part = pack_rows(keyres[:, block_of(p), c * chunk : (c + 1) * chunk])
                res_out[p, c] = part.astype(BF16)
    for c in range(chunks):
        for peer in peers:
            remote(
                res_out.at[peer, c],
                res_pix[c].at[pl.ds(me * slots, slots)],
                send.at[3],
                res_recv.at[c],
                frame=peer,
            ).start()
    for c in range(chunks):
        res_pix[c][pl.ds(me * slots, slots)] = res_out[me, c]

    with jax.named_scope("w_loads"):
        for load in loads[4:]:
            load.wait()
    with jax.named_scope("w_lat"):
        drain(lat_pix.at[: (n - 1) * frames_dev], lat_recv.at[0])

    small = frames <= 24
    block = frames * group
    factor = math.log2(math.e) / math.sqrt(head_dim)
    encode = encoding[...][:, None, :]
    lane = lax.broadcasted_iota(jnp.int32, (1, 128), 1)
    pairs_total = HEADS // 2

    def soft(values):
        width = values.shape[-1]
        values = values.reshape(frames, group, width)
        top = jnp.max(values, axis=0, keepdims=True)
        powers = jnp.exp2(values - top)
        total = jnp.sum(powers, axis=0, keepdims=True)
        pixel = lax.broadcasted_iota(jnp.int32, (1, group, width), 1)
        query = lax.broadcasted_iota(jnp.int32, (1, group, width), 2)
        weight = jnp.where(lax.rem(query, group) == pixel, 1.0 / total, 0.0)
        return (powers * weight).reshape(block, width).astype(BF16)

    def hide(c):
        span = slice(c * chunk, (c + 1) * chunk)
        drain(res_pix[c].at[: (n - 1) * slots], res_recv.at[c])

        def one(f, carry):
            slot = propagate[f]
            gap = jnp.abs(f - key_frames[slot]).astype(F32)
            reach = jnp.exp(jnp.full((1, channels), -gap / (2 * frames_dev), F32))
            residual = unpack_rows(res_pix[c], slot, chunk, channels, 0, chunk)
            value = unpack_rows(lat_pix, f, pix, channels, c * chunk, chunk) + reach * residual
            hidden[f, span] = value
            return carry

        lax.fori_loop(0, frames, one, 0, unroll=small)

    mask = jnp.where(lane < head_dim, 1.0, 0.0).astype(BF16)
    other = jnp.where(lane < head_dim, 0.0, 1.0).astype(BF16)

    def prepare(s):
        base = hidden[:, s * group : (s + 1) * group]
        value = norm(base, gain_a[...]) + encode
        normed[s % 2] = value.reshape(block, channels).astype(BF16)

    def project_q(s, t):
        query = dot(normed[s % 2], q_wp[:, 256 * t : 256 * (t + 1)]) * factor
        query = query.astype(BF16)
        for i in range(2):
            tile = query[:, 128 * i : 128 * (i + 1)]
            q_both[s % 2, 2 * t + i, :block] = tile * mask
            q_both[s % 2, 2 * t + i, block:] = tile * other

    def project_k(s, t):
        keys = dot(normed[s % 2], k_wp[:, 256 * t : 256 * (t + 1)])
        k_held[s % 2, :, 256 * t : 256 * (t + 1)] = keys.astype(BF16)

    def project_v(s):
        v_held[s % 2] = dot_nt(v_wt[...], normed[s % 2]).astype(BF16)

    def project(s):
        prepare(s)
        for t in range(pairs_total // 2):
            project_q(s, t)
            project_k(s, t)
        project_v(s)

    def score(s, j):
        keys = k_held[s % 2, :, 128 * j : 128 * (j + 1)]
        scores[j % 2] = dot_nt(keys, q_both[s % 2, j])

    def soften(s, j, low, high):
        probs[j % 2, :, low:high] = soft(scores[j % 2, :, low:high])

    def mix(s, j):
        low, high = 2 * j * head_dim, 2 * (j + 1) * head_dim
        pair = dot(v_held[s % 2, low:high], probs[j % 2])
        mixed_t[low : low + head_dim] = pair[:head_dim, :block]
        mixed_t[low + head_dim : high] = pair[head_dim:, block:]

    def finish(s):
        mixed = jnp.transpose(mixed_t[...]).astype(BF16)
        projected = dot(mixed, squares[4]).reshape(frames, group, channels)
        base = hidden[:, s * group : (s + 1) * group]
        total = base + projected
        for p in range(n):
            part = pack_lead(total[p * frames_dev : (p + 1) * frames_dev])
            att_out[s, p] = part.astype(BF16)
        for peer in peers:
            remote(
                att_out.at[s, peer],
                att_in.at[me, s],
                send.at[4],
                att_recv.at[s, (lax.div(peer, rows) != home).astype(jnp.int32)],
                frame=peer,
            ).start()
        att_in[me, s] = att_out[s, me]

    def activate_block(s, block):
        taken = [
            unpack_lead(att_in[block * rows + r, s].astype(F32), frames_dev, channels)
            for r in range(rows)
        ]
        value = jnp.stack(taken, axis=1)
        active = silu(norm(value, gain_c[...]))
        act_out[0, s, block] = pack_lead(active[:, 0]).astype(BF16)
        act_out[1, s, block] = pack_lead(active[:, rows - 1]).astype(BF16)
        which = 1 if s == pieces - 1 else 0
        act_up = up(
            act_out.at[0, s, block], act_bot.at[s, block], send.at[5], ah_recv.at[0, which]
        )
        act_down = down(
            act_out.at[1, s, block], act_top.at[s, block], send.at[6], ah_recv.at[1, which]
        )
        pl.when(has_up)(act_up.start)
        pl.when(has_down)(act_down.start)
        att[:, :, block, s] = value.astype(BF16)
        act[:, :, block, s] = active.astype(BF16)

    def activate_home(s):
        if rows > 1:
            drain(att_in.at[: rows - 1, s], att_recv.at[s, 0])
        activate_block(s, home)

    def activate_rest(s):
        drain(att_in.at[: n - rows, s], att_recv.at[s, 1])
        for i in range(1, per_row):
            activate_block(s, lax.rem(home + i, per_row))

    def activate(s):
        with jax.named_scope(f"home{s}"):
            activate_home(s)
        with jax.named_scope(f"rest{s}"):
            activate_rest(s)

    def attend_all():
        turns = [(s, j) for s in range(pieces) for j in range(pairs_total)]
        tiles = [(low, min(low + 128, 2 * block)) for low in range(0, 2 * block, 128)]
        hide(0)
        project(0)
        score(0, 0)
        for k, (s, j) in enumerate(turns):
            work = []
            if k > 0:
                work.append(functools.partial(mix, *turns[k - 1]))
            if k + 1 < len(turns) and j + 1 < pairs_total:
                work.append(functools.partial(score, s, j + 1))
            if j == 0 and s > 0:
                work.append(functools.partial(finish, s - 1))
            if s + 1 < pieces:
                if j == 1:
                    if (s + 1) % per_chunk == 0:
                        hide((s + 1) // per_chunk)
                    work.append(functools.partial(prepare, s + 1))
                    work.append(functools.partial(project_q, s + 1, 0))
                if j == 2:
                    work.append(functools.partial(project_q, s + 1, 1))
                    work.append(functools.partial(project_k, s + 1, 0))
                if j == 3:
                    work.append(functools.partial(project_k, s + 1, 1))
                    work.append(functools.partial(project_v, s + 1))
                    work.append(functools.partial(score, s + 1, 0))
            for i in range(max(len(tiles), len(work))):
                if i < len(tiles):
                    soften(s, j, *tiles[i])
                if i < len(work):
                    work[i]()
            if (pieces - s, j) == (1, 3) and pieces > 1:
                activate(0)
        mix(*turns[-1])
        finish(pieces - 1)

    with jax.named_scope("attention"):
        if small:
            attend_all()
        else:
            for s in range(pieces):
                if s % per_chunk == 0:
                    hide(s // per_chunk)
                project(s)

                def step(j, carry):
                    keys = k_held[s % 2, :, pl.ds(pl.multiple_of(128 * j, 128), 128)]
                    for i in range(2):
                        part = q_both[s % 2, j, i * block : (i + 1) * block]
                        row = pl.ds(pl.multiple_of((2 * j + i) * head_dim, 8), head_dim)
                        value = dot(v_held[s % 2], soft(dot_nt(keys, part)))
                        scores[0, :channels, :block] = value
                        mixed_t[row] = scores[0, row, :block]
                    return carry

                lax.fori_loop(0, pairs_total, step, 0)
                finish(s)

    def add_b(r, span, ref, taps):
        parts = []
        for s in range(span.start, span.stop):
            taken = [
                unpack_lead(ref[s, q].astype(F32), frames_dev, channels) for q in range(per_row)
            ]
            parts.append(jnp.stack(taken, axis=1).reshape(-1, channels).astype(BF16))
        value = dot(jnp.concatenate(parts, axis=0), taps)
        value = value.reshape(len(parts), frames_dev, per_row, group, value.shape[-1])
        for i, s in enumerate(range(span.start, span.stop)):
            sums_b[:, r, :, s] += value[i]

    def put_all(r, value):
        sums_b[:, r] = value.reshape(frames_dev, -1, per_row, pieces, group, value.shape[-1])

    def add_all(r, value):
        sums_b[:, r] += value.reshape(frames_dev, -1, per_row, pieces, group, value.shape[-1])

    early = 1 if small and pieces > 1 else 0
    for s in range(early, pieces):
        activate(s)
    wait_taps(blk_w, w_sem.at[1])
    with jax.named_scope("blkconv_local"):
        conv_local(act[...].reshape(frames_dev, rows, -1, group, channels), blk_w, put_all, add_all)
    last = max(pieces - 1, 0)
    for span in [slice(0, last), slice(last, pieces)] if last else [slice(0, pieces)]:
        with jax.named_scope(f"w_acthalo{span.start}"):
            which = 1 if span.stop == pieces else 0
            pl.when(has_up)(lambda: drain(act_top.at[span], ah_recv.at[1, which]))
            pl.when(has_down)(lambda: drain(act_bot.at[span], ah_recv.at[0, which]))
        with jax.named_scope(f"blkconv_edge{span.start}"):
            add_b(0, span, act_top, blk_w[0])
            add_b(rows - 1, span, act_bot, blk_w[2])
    with jax.named_scope("w_end"):
        pl.when(has_up)(cond_up.wait_send)
        pl.when(has_down)(cond_down.wait_send)
        drain(lat_pix.at[: (n - 1) * frames_dev], send.at[2])
        drain(res_out.at[: n - 1], send.at[3])
        drain(att_out.at[:, : n - 1], send.at[4])
        pl.when(has_up)(lambda: drain(act_out.at[0], send.at[5]))
        pl.when(has_down)(lambda: drain(act_out.at[1], send.at[6]))


def add_up(main, tail, sums, att, out_hbm, out, sem):
    frames_dev, rows, cols, channels = out.shape
    stores = []
    for f in range(frames_dev):
        for r in range(rows):
            convolved = conv_row(sums[f, r].reshape(cols, -1), main, tail)
            held = att[f, r].astype(F32).reshape(cols, channels)
            out[f, r] = (held + convolved).astype(BF16)
        stores.append(pltpu.make_async_copy(out.at[f], out_hbm.at[f], sem.at[f]))
        stores[f].start()
    for store in stores:
        store.wait()


def shards(
    latents,
    condition,
    key_frames,
    propagate,
    encoder_conv,
    zero_conv,
    attention_gain,
    query_weight,
    key_weight,
    value_weight,
    output_weight,
    conv_gain,
    block_conv,
):
    frames_dev, rows, cols, channels = latents.shape
    slots = condition.shape[0]
    n = lax.axis_size("frame")
    row_total = lax.axis_size("row")
    pix = rows * cols // n
    frames = frames_dev * n
    chunk = 16 if pix % 16 == 0 else 8
    chunks = pix // chunk
    group = 8
    pieces = pix // group
    block = frames * group
    per_row = n // rows
    main = channels // 256 * 256
    tail = channels - main
    wide = 3 * (main + tail)
    lat_size = packed_size(pix, channels)
    res_size = packed_size(chunk, channels)
    cond_size = packed_size(cols, channels)
    att_size = frames_dev * (channels // 128) + frames_dev // 2
    encoding = jnp.asarray(positions(frames, channels))
    square = (channels, channels)
    dma = pltpu.SemaphoreType.DMA
    values = [
        latents.reshape(frames_dev, n, pix, channels),
        condition,
        key_frames,
        propagate,
        encoding,
        attention_gain,
        conv_gain,
        encoder_conv,
        zero_conv,
        query_weight,
        key_weight,
        value_weight,
        output_weight,
        block_conv,
    ]
    values = [pltpu.with_memory_space_constraint(v, pltpu.MemorySpace.HBM) for v in values]
    sums_shape = pltpu.VMEM((frames_dev, rows, per_row, pieces, group, wide), F32)
    att_shape = pltpu.VMEM((frames_dev, rows, per_row, pieces, group, channels), BF16)
    vmem = pl.BlockSpec(memory_space=pltpu.VMEM)
    sums, att = pl.pallas_call(
        functools.partial(kernel, n, row_total),
        out_shape=(sums_shape, att_shape),
        in_specs=[pl.BlockSpec(memory_space=pl.ANY)] * len(values),
        out_specs=(vmem, vmem),
        scratch_shapes=[
            pltpu.SMEM(key_frames.shape, jnp.int32),
            pltpu.SMEM(propagate.shape, jnp.int32),
            pltpu.VMEM((frames, channels), F32),
            pltpu.VMEM((channels,), F32),
            pltpu.VMEM((channels,), F32),
            pltpu.VMEM(condition.shape, BF16),
            pltpu.VMEM((3, channels, wide), BF16),
            pltpu.VMEM((9, channels, tail), BF16),
            pltpu.VMEM((5,) + square, BF16),
            pltpu.VMEM((3, channels, wide), BF16),
            pltpu.VMEM((9, channels, tail), BF16),
            pltpu.VMEM(square, BF16),
            pltpu.VMEM((channels, 64 * HEADS), BF16),
            pltpu.VMEM((channels, 64 * HEADS), BF16),
            pltpu.VMEM((2, block, channels), BF16),
            pltpu.VMEM((2, HEADS // 2, 2 * block, 128), BF16),
            pltpu.VMEM((2, block, 64 * HEADS), BF16),
            pltpu.VMEM((2, channels, block), BF16),
            pltpu.VMEM((2, block, 2 * block), F32),
            pltpu.VMEM((2, block, 2 * block), BF16),
            pltpu.VMEM((channels, block), F32),
            pltpu.VMEM((frames_dev, n, pix, channels), BF16),
            pltpu.VMEM((n, frames_dev, lat_size, 128), BF16),
            pltpu.VMEM((frames, lat_size, 128), BF16),
            pltpu.VMEM((n, chunks, slots, res_size, 128), BF16),
            [pltpu.VMEM((slots * n, res_size, 128), BF16) for _ in range(chunks)],
            pltpu.VMEM((frames, pix, channels), F32),
            pltpu.VMEM((pieces, n, att_size, group, 128), BF16),
            pltpu.VMEM((n, pieces, att_size, group, 128), BF16),
            pltpu.VMEM((frames_dev, rows, per_row, pieces, group, channels), BF16),
            pltpu.VMEM((2, slots, cond_size, 128), BF16),
            pltpu.VMEM((slots, cond_size, 128), BF16),
            pltpu.VMEM((slots, cond_size, 128), BF16),
            pltpu.VMEM((2, pieces, per_row, att_size, group, 128), BF16),
            pltpu.VMEM((pieces, per_row, att_size, group, 128), BF16),
            pltpu.VMEM((pieces, per_row, att_size, group, 128), BF16),
            pltpu.VMEM((slots, rows, cols, wide), F32),
            dma((12,)),
            dma((7,)),
            dma((1,)),
            dma((chunks,)),
            dma((pieces, 2)),
            dma((2,)),
            dma((2, 2)),
        ],
        compiler_params=pltpu.CompilerParams(
            collective_id=0, has_side_effects=True, vmem_limit_bytes=48 * 1024 * 1024
        ),
    )(*values)
    return pl.pallas_call(
        functools.partial(add_up, main, tail),
        out_shape=jax.ShapeDtypeStruct(latents.shape, BF16),
        in_specs=[vmem, vmem],
        out_specs=pl.BlockSpec(memory_space=pl.ANY),
        scratch_shapes=[pltpu.VMEM(latents.shape, BF16), dma((frames_dev,))],
        compiler_params=pltpu.CompilerParams(vmem_limit_bytes=4 * 1024 * 1024),
    )(sums, att)


def solution(mesh):
    placed = (
        P(("group", "frame"), "row", None, None),
        P(("group", "frame"), "row", None, None),
        P("group"),
        P("group"),
        P(),
        P(),
        P(),
        P(),
        P(),
        P(),
        P(),
        P(),
        P(),
    )
    return jax.shard_map(
        shards,
        mesh=mesh,
        in_specs=placed,
        out_specs=P(("group", "frame"), "row", None, None),
        check_vma=False,
    )
```

```python
import functools
import math

import jax
import jax.numpy as jnp
import numpy as np
from jax import lax
from jax.experimental import pallas as pl
from jax.experimental.pallas import tpu as pltpu
from jax.sharding import PartitionSpec as P

HEADS = 8
MESH = pl.DeviceIdType.MESH
F32 = jnp.float32
BF16 = jnp.bfloat16


def positions(frame_total, channels):
    frame_pos = np.arange(frame_total, dtype=np.float64)[:, None]
    half_index = np.arange(channels // 2, dtype=np.float64)
    frequency = np.exp(half_index * (-2.0 * math.log(10000.0) / channels))
    angles = frame_pos * frequency
    stacked = np.stack([np.sin(angles), np.cos(angles)], axis=-1)
    return stacked.reshape(frame_total, channels).astype(np.float32)


def norm(values, gain):
    average = jnp.mean(values, axis=-1, keepdims=True)
    centered = values - average
    variance = jnp.mean(centered * centered, axis=-1, keepdims=True)
    return centered * lax.rsqrt(variance + 1e-05) * gain


def silu(values):
    half = 0.5 * values
    return half + half * jnp.tanh(half)


def dot(left, right):
    return jnp.dot(left, right, preferred_element_type=F32)


def dot_nt(left, right):
    return lax.dot_general(left, right, (((1,), (1,)), ((), ())), preferred_element_type=F32)


def flat(values):
    return values.astype(F32).reshape(-1, values.shape[-1]).astype(BF16)


def pack_rows(values):
    size = values.shape[1]
    whole = values.shape[2] // 128 * 128
    parts = [values[:, :, low : low + 128] for low in range(0, whole, 128)]
    tail = values[:, :, whole:]
    if size % 16 == 0:
        parts.append(jnp.concatenate([tail[:, : size // 2], tail[:, size // 2 :]], axis=2))
    else:
        parts.append(jnp.concatenate([tail, jnp.zeros_like(tail)], axis=2))
    return jnp.concatenate(parts, axis=1)


def packed_size(size, channels):
    return size * (channels // 128) + (size // 2 if size % 16 == 0 else size)


def unpack_rows(ref, index, size, channels, low, count):
    whole = channels // 128
    rest = channels - whole * 128
    def take(start, rows):
        if isinstance(index, tuple):
            return ref[index[0], :, start : start + rows].astype(F32)
        return ref[index, start : start + rows].astype(F32)

    parts = [take(i * size + low, count) for i in range(whole)]
    if size % 16:
        tail = take(whole * size + low, count)[..., :rest]
    else:
        half = size // 2
        start = low % half
        tile = take(whole * size + start, min(count, half))
        if count == size:
            tail = jnp.concatenate([tile[..., :rest], tile[..., rest:]], axis=-2)
        else:
            tail = tile[..., :rest] if low < half else tile[..., rest:]
    return jnp.concatenate(parts + [tail], axis=-1)


def pack_lead(values):
    count = values.shape[0]
    whole = values.shape[2] // 128 * 128
    parts = [values[:, :, low : low + 128] for low in range(0, whole, 128)]
    tail = values[:, :, whole:]
    parts.append(jnp.concatenate([tail[: count // 2], tail[count // 2 :]], axis=2))
    return jnp.concatenate(parts, axis=0)


def unpack_lead(values, count, channels):
    whole = channels // 128
    rest = channels - whole * 128
    parts = [values[i * count : (i + 1) * count] for i in range(whole)]
    tile = values[whole * count :]
    parts.append(jnp.concatenate([tile[..., :rest], tile[..., rest:]], axis=0))
    return jnp.concatenate(parts, axis=-1)


def pack_tails(tails, packed, main):
    wide = 3 * main
    for a in range(3):
        parts = [tails[3 * a + b] for b in range(3)]
        packed[a, :, wide:] = jnp.concatenate(parts, axis=1)


def conv_local(images, packed, put, add):
    rows = images.shape[1]
    put(slice(0, rows), dot(flat(images), packed[1]))
    if rows > 1:
        add(slice(1, rows), dot(flat(images[:, : rows - 1]), packed[0]))
        add(slice(0, rows - 1), dot(flat(images[:, 1:]), packed[2]))


def pair_tiles(weight, width):
    rows, channels = weight.shape
    tiles = []
    for low in range(0, channels, width):
        tiles.append(weight[:, low : low + width])
        tiles.append(jnp.zeros((rows, 128 - width), weight.dtype))
    return jnp.concatenate(tiles, axis=1)


def conv_row(total, main, tail):
    cols = total.shape[0]
    col = lax.broadcasted_iota(jnp.int32, (cols, 1), 0)
    pieces = []
    for start, size in ((0, main), (3 * main, tail)):
        left, middle, right = (total[:, start + b * size : start + (b + 1) * size] for b in range(3))
        left = jnp.where(col == 0, 0.0, pltpu.roll(left, 1, 0))
        right = jnp.where(col == cols - 1, 0.0, pltpu.roll(right, cols - 1, 0))
        pieces.append(left + middle + right)
    return jnp.concatenate(pieces, axis=1)


def kernel(
    n,
    row_total,
    lat,
    cond_hbm,
    key_hbm,
    prop_hbm,
    encoding_hbm,
    gain_a_hbm,
    gain_c_hbm,
    enc_hbm,
    zero_hbm,
    q_hbm,
    k_hbm,
    v_hbm,
    o_hbm,
    blk_hbm,
    sums_b,
    att,
    key_frames,
    propagate,
    encoding,
    gain_a,
    gain_c,
    cond,
    enc_w,
    enc_t,
    squares,
    blk_w,
    blk_t,
    v_wt,
    q_wp,
    k_wp,
    normed,
    q_both,
    k_held,
    v_held,
    scores,
    probs,
    mixed_t,
    lat_own,
    lat_out,
    lat_pix,
    res_out,
    res_pix,
    hidden,
    att_out,
    att_in,
    act,
    cond_out,
    cond_top,
    cond_bot,
    act_out,
    act_top,
    act_bot,
    sums_e,
    w_sem,
    send,
    lat_recv,
    res_recv,
    att_recv,
    ch_recv,
    ah_recv,
):
    me = lax.axis_index("frame")
    row_me = lax.axis_index("row")
    frames_dev, _, pix, channels = lat.shape
    slots, rows, cols, _ = cond.shape
    chunks = res_recv.shape[0]
    chunk = pix // chunks
    frames = hidden.shape[0]
    pieces, group = att.shape[3:5]
    per_chunk = chunk // group
    per_row = n // rows
    head_dim = channels // HEADS
    main = enc_w.shape[2] // 3 // 128 * 128
    tail = channels - main
    def block_of(p):
        return p % rows * per_row + p // rows

    home = lax.div(me, rows)
    has_up = row_me > 0
    has_down = row_me < row_total - 1

    barrier = pltpu.get_barrier_semaphore()
    for k in range(1, n):
        pl.semaphore_signal(
            barrier, inc=1, device_id={"frame": lax.rem(me + k, n)}, device_id_type=MESH
        )

    @pl.when(has_up)
    def _():
        pl.semaphore_signal(barrier, inc=1, device_id={"row": row_me - 1}, device_id_type=MESH)

    @pl.when(has_down)
    def _():
        pl.semaphore_signal(barrier, inc=1, device_id={"row": row_me + 1}, device_id_type=MESH)

    def start_taps(src, packed, sem):
        for a in range(3):
            for b in range(3):
                pltpu.make_async_copy(
                    src.at[3 * a + b, :, :main], packed.at[a, :, b * main : (b + 1) * main], sem
                ).start()

    def wait_taps(packed, sem):
        whole = packed.at[:, :, : 3 * main]
        pltpu.make_async_copy(whole, whole, sem).wait()

    pairs = [
        (cond_hbm, cond),
        (lat, lat_own),
        (enc_hbm.at[:, :, main:], enc_t),
        (blk_hbm.at[:, :, main:], blk_t),
        (encoding_hbm, encoding),
        (gain_a_hbm, gain_a),
        (gain_c_hbm, gain_c),
        (key_hbm, key_frames),
        (prop_hbm, propagate),
    ]
    loads = [pltpu.make_async_copy(s, d, w_sem.at[3 + i]) for i, (s, d) in enumerate(pairs)]
    loads[0].start()
    loads[1].start()
    loads[2].start()

    @pl.when(jnp.logical_not(has_up))
    def _():
        cond_top[...] = jnp.zeros_like(cond_top)
        act_top[...] = jnp.zeros_like(act_top)

    @pl.when(jnp.logical_not(has_down))
    def _():
        cond_bot[...] = jnp.zeros_like(cond_bot)
        act_bot[...] = jnp.zeros_like(act_bot)

    start_taps(enc_hbm, enc_w, w_sem.at[0])
    loads[0].wait()
    cond_out[0] = pack_rows(cond[:, 0].astype(F32)).astype(BF16)
    cond_out[1] = pack_rows(cond[:, rows - 1].astype(F32)).astype(BF16)
    neighbours = has_up.astype(jnp.int32) + has_down.astype(jnp.int32)
    with jax.named_scope("w_barrier"):
        pl.semaphore_wait(barrier, n - 1 + neighbours)

    def remote(src, dst, send_sem, recv_sem, **where):
        return pltpu.make_async_remote_copy(
            src_ref=src,
            dst_ref=dst,
            send_sem=send_sem,
            recv_sem=recv_sem,
            device_id=where,
            device_id_type=MESH,
        )

    def up(src, dst, send_sem, recv_sem):
        return remote(src, dst, send_sem, recv_sem, row=row_me - 1)

    def down(src, dst, send_sem, recv_sem):
        return remote(src, dst, send_sem, recv_sem, row=row_me + 1)

    def drain(ref, sem):
        pltpu.make_async_copy(ref, ref, sem).wait()

    cond_up = up(cond_out.at[0], cond_bot, send.at[0], ch_recv.at[0])
    cond_down = down(cond_out.at[1], cond_top, send.at[1], ch_recv.at[1])
    pl.when(has_up)(cond_up.start)
    pl.when(has_down)(cond_down.start)

    loads[1].wait()
    for p in range(n):
        lat_out[p] = pack_rows(lat_own[:, block_of(p)].astype(F32)).astype(BF16)
    peers = [lax.rem(me + k, n) for k in range(1, n)]
    for peer in peers:
        remote(
            lat_out.at[peer],
            lat_pix.at[pl.ds(me * frames_dev, frames_dev)],
            send.at[2],
            lat_recv.at[0],
            frame=peer,
        ).start()
    lat_pix[pl.ds(me * frames_dev, frames_dev)] = lat_out[me]
    for i, source in enumerate((v_hbm, zero_hbm, q_hbm, k_hbm, o_hbm)):
        pltpu.make_async_copy(source, squares.at[i], w_sem.at[2]).start()
    for load in loads[3:]:
        load.start()
    start_taps(blk_hbm, blk_w, w_sem.at[1])

    with jax.named_scope("w_load01"):
        loads[2].wait()
    with jax.named_scope("pack_enc"):
        pack_tails(enc_t, enc_w, main)
        wait_taps(enc_w, w_sem.at[0])

    def edge_rows(ref, index, size):
        values = unpack_rows(ref, index, size, channels, 0, size)
        return values.reshape(-1, channels).astype(BF16)

    def put_e(r, value):
        sums_e[:, r] = value.reshape(slots, -1, cols, value.shape[-1])

    def add_e(r, value):
        sums_e[:, r] += value.reshape(slots, -1, cols, value.shape[-1])

    with jax.named_scope("encconv_local"):
        conv_local(cond[...], enc_w, put_e, add_e)
    with jax.named_scope("prep"):
        drain(squares, w_sem.at[2])
        v_wt[...] = jnp.transpose(squares[0].astype(F32)).astype(BF16)
        q_wp[...] = pair_tiles(squares[2], 2 * head_dim)
        k_wp[...] = pair_tiles(squares[3], 2 * head_dim)
        loads[3].wait()
        pack_tails(blk_t, blk_w, main)
    with jax.named_scope("w_condhalo"):
        pl.when(has_up)(cond_down.wait_recv)
        pl.when(has_down)(cond_up.wait_recv)
    with jax.named_scope("encconv_edge"):
        add_e(slice(0, 1), dot(edge_rows(cond_top, slice(None), cols), enc_w[0]))
        add_e(slice(rows - 1, rows), dot(edge_rows(cond_bot, slice(None), cols), enc_w[2]))
    with jax.named_scope("enc_silu_zero"):
        encoded = jnp.concatenate(
            [silu(conv_row(sums_e[s, r], main, tail)) for s in range(slots) for r in range(rows)],
            axis=0,
        ).astype(BF16)
        keyres = dot(encoded, squares[1]).reshape(slots, n, pix, channels)
        for p in range(n):
            for c in range(chunks):
                part = pack_rows(keyres[:, block_of(p), c * chunk : (c + 1) * chunk])
                res_out[p, c] = part.astype(BF16)
    for c in range(chunks):
        for peer in peers:
            remote(
                res_out.at[peer, c],
                res_pix[c].at[pl.ds(me * slots, slots)],
                send.at[3],
                res_recv.at[c],
                frame=peer,
            ).start()
    for c in range(chunks):
        res_pix[c][pl.ds(me * slots, slots)] = res_out[me, c]

    with jax.named_scope("w_loads"):
        for load in loads[4:]:
            load.wait()
    with jax.named_scope("w_lat"):
        drain(lat_pix.at[: (n - 1) * frames_dev], lat_recv.at[0])

    small = frames <= 24
    block = frames * group
    factor = math.log2(math.e) / math.sqrt(head_dim)
    encode = encoding[...][:, None, :]
    lane = lax.broadcasted_iota(jnp.int32, (1, 128), 1)
    pairs_total = HEADS // 2

    def soft(values):
        width = values.shape[-1]
        values = values.reshape(frames, group, width)
        top = jnp.max(values, axis=0, keepdims=True)
        powers = jnp.exp2(values - top)
        total = jnp.sum(powers, axis=0, keepdims=True)
        pixel = lax.broadcasted_iota(jnp.int32, (1, group, width), 1)
        query = lax.broadcasted_iota(jnp.int32, (1, group, width), 2)
        weight = jnp.where(lax.rem(query, group) == pixel, 1.0 / total, 0.0)
        return (powers * weight).reshape(block, width).astype(BF16)

    def hide(c):
        span = slice(c * chunk, (c + 1) * chunk)
        drain(res_pix[c].at[: (n - 1) * slots], res_recv.at[c])

        def one(f, carry):
            slot = propagate[f]
            gap = jnp.abs(f - key_frames[slot]).astype(F32)
            reach = jnp.exp(jnp.full((1, channels), -gap / (2 * frames_dev), F32))
            residual = unpack_rows(res_pix[c], slot, chunk, channels, 0, chunk)
            value = unpack_rows(lat_pix, f, pix, channels, c * chunk, chunk) + reach * residual
            hidden[f, span] = value
            return carry

        lax.fori_loop(0, frames, one, 0, unroll=small)

    mask = jnp.where(lane < head_dim, 1.0, 0.0).astype(BF16)
    other = jnp.where(lane < head_dim, 0.0, 1.0).astype(BF16)

    def prepare(s):
        base = hidden[:, s * group : (s + 1) * group]
        value = norm(base, gain_a[...]) + encode
        normed[s % 2] = value.reshape(block, channels).astype(BF16)

    def project_q(s, t):
        query = dot(normed[s % 2], q_wp[:, 256 * t : 256 * (t + 1)]) * factor
        query = query.astype(BF16)
        for i in range(2):
            tile = query[:, 128 * i : 128 * (i + 1)]
            q_both[s % 2, 2 * t + i, :block] = tile * mask
            q_both[s % 2, 2 * t + i, block:] = tile * other

    def project_k(s, t):
        keys = dot(normed[s % 2], k_wp[:, 256 * t : 256 * (t + 1)])
        k_held[s % 2, :, 256 * t : 256 * (t + 1)] = keys.astype(BF16)

    def project_v(s):
        v_held[s % 2] = dot_nt(v_wt[...], normed[s % 2]).astype(BF16)

    def project(s):
        prepare(s)
        for t in range(pairs_total // 2):
            project_q(s, t)
            project_k(s, t)
        project_v(s)

    def score(s, j):
        keys = k_held[s % 2, :, 128 * j : 128 * (j + 1)]
        scores[j % 2] = dot_nt(keys, q_both[s % 2, j])

    def soften(s, j, low, high):
        probs[j % 2, :, low:high] = soft(scores[j % 2, :, low:high])

    def mix(s, j):
        low, high = 2 * j * head_dim, 2 * (j + 1) * head_dim
        pair = dot(v_held[s % 2, low:high], probs[j % 2])
        mixed_t[low : low + head_dim] = pair[:head_dim, :block]
        mixed_t[low + head_dim : high] = pair[head_dim:, block:]

    def finish(s):
        mixed = jnp.transpose(mixed_t[...]).astype(BF16)
        projected = dot(mixed, squares[4]).reshape(frames, group, channels)
        base = hidden[:, s * group : (s + 1) * group]
        total = base + projected
        for p in range(n):
            part = pack_lead(total[p * frames_dev : (p + 1) * frames_dev])
            att_out[s, p] = part.astype(BF16)
        for peer in peers:
            remote(
                att_out.at[s, peer],
                att_in.at[me, s],
                send.at[4],
                att_recv.at[s, (lax.div(peer, rows) != home).astype(jnp.int32)],
                frame=peer,
            ).start()
        att_in[me, s] = att_out[s, me]

    def activate_block(s, block):
        taken = [
            unpack_lead(att_in[block * rows + r, s].astype(F32), frames_dev, channels)
            for r in range(rows)
        ]
        value = jnp.stack(taken, axis=1)
        active = silu(norm(value, gain_c[...]))
        act_out[0, s, block] = pack_lead(active[:, 0]).astype(BF16)
        act_out[1, s, block] = pack_lead(active[:, rows - 1]).astype(BF16)
        which = 1 if s == pieces - 1 else 0
        act_up = up(
            act_out.at[0, s, block], act_bot.at[s, block], send.at[5], ah_recv.at[0, which]
        )
        act_down = down(
            act_out.at[1, s, block], act_top.at[s, block], send.at[6], ah_recv.at[1, which]
        )
        pl.when(has_up)(act_up.start)
        pl.when(has_down)(act_down.start)
        att[:, :, block, s] = value.astype(BF16)
        act[:, :, block, s] = active.astype(BF16)

    def activate_home(s):
        if rows > 1:
            drain(att_in.at[: rows - 1, s], att_recv.at[s, 0])
        activate_block(s, home)

    def activate_rest(s):
        drain(att_in.at[: n - rows, s], att_recv.at[s, 1])
        for i in range(1, per_row):
            activate_block(s, lax.rem(home + i, per_row))

    def activate(s):
        with jax.named_scope(f"home{s}"):
            activate_home(s)
        with jax.named_scope(f"rest{s}"):
            activate_rest(s)

    def attend_all():
        turns = [(s, j) for s in range(pieces) for j in range(pairs_total)]
        tiles = [(low, min(low + 128, 2 * block)) for low in range(0, 2 * block, 128)]
        hide(0)
        project(0)
        score(0, 0)
        for k, (s, j) in enumerate(turns):
            work = []
            if k > 0:
                work.append(functools.partial(mix, *turns[k - 1]))
            if k + 1 < len(turns) and j + 1 < pairs_total:
                work.append(functools.partial(score, s, j + 1))
            if j == 0 and s > 0:
                work.append(functools.partial(finish, s - 1))
            if s + 1 < pieces:
                if j == 1:
                    if (s + 1) % per_chunk == 0:
                        hide((s + 1) // per_chunk)
                    work.append(functools.partial(prepare, s + 1))
                    work.append(functools.partial(project_q, s + 1, 0))
                if j == 2:
                    work.append(functools.partial(project_q, s + 1, 1))
                    work.append(functools.partial(project_k, s + 1, 0))
                if j == 3:
                    work.append(functools.partial(project_k, s + 1, 1))
                    work.append(functools.partial(project_v, s + 1))
                    work.append(functools.partial(score, s + 1, 0))
            for i in range(max(len(tiles), len(work))):
                if i < len(tiles):
                    soften(s, j, *tiles[i])
                if i < len(work):
                    work[i]()
            if (pieces - s, j) == (1, 3) and pieces > 1:
                activate(0)
        mix(*turns[-1])
        finish(pieces - 1)

    with jax.named_scope("attention"):
        if small:
            attend_all()
        else:
            for s in range(pieces):
                if s % per_chunk == 0:
                    hide(s // per_chunk)
                project(s)

                def step(j, carry):
                    keys = k_held[s % 2, :, pl.ds(pl.multiple_of(128 * j, 128), 128)]
                    for i in range(2):
                        part = q_both[s % 2, j, i * block : (i + 1) * block]
                        row = pl.ds(pl.multiple_of((2 * j + i) * head_dim, 8), head_dim)
                        value = dot(v_held[s % 2], soft(dot_nt(keys, part)))
                        scores[0, :channels, :block] = value
                        mixed_t[row] = scores[0, row, :block]
                    return carry

                lax.fori_loop(0, pairs_total, step, 0)
                finish(s)

    def add_b(r, span, ref, taps):
        parts = []
        for s in range(span.start, span.stop):
            taken = [
                unpack_lead(ref[s, q].astype(F32), frames_dev, channels) for q in range(per_row)
            ]
            parts.append(jnp.stack(taken, axis=1).reshape(-1, channels).astype(BF16))
        value = dot(jnp.concatenate(parts, axis=0), taps)
        value = value.reshape(len(parts), frames_dev, per_row, group, value.shape[-1])
        for i, s in enumerate(range(span.start, span.stop)):
            sums_b[:, r, :, s] += value[i]

    def put_all(r, value):
        sums_b[:, r] = value.reshape(frames_dev, -1, per_row, pieces, group, value.shape[-1])

    def add_all(r, value):
        sums_b[:, r] += value.reshape(frames_dev, -1, per_row, pieces, group, value.shape[-1])

    early = 1 if small and pieces > 1 else 0
    for s in range(early, pieces):
        activate(s)
    wait_taps(blk_w, w_sem.at[1])
    with jax.named_scope("blkconv_local"):
        conv_local(act[...].reshape(frames_dev, rows, -1, group, channels), blk_w, put_all, add_all)
    last = max(pieces - 1, 0)
    for span in [slice(0, last), slice(last, pieces)] if last else [slice(0, pieces)]:
        with jax.named_scope(f"w_acthalo{span.start}"):
            which = 1 if span.stop == pieces else 0
            pl.when(has_up)(lambda: drain(act_top.at[span], ah_recv.at[1, which]))
            pl.when(has_down)(lambda: drain(act_bot.at[span], ah_recv.at[0, which]))
        with jax.named_scope(f"blkconv_edge{span.start}"):
            add_b(0, span, act_top, blk_w[0])
            add_b(rows - 1, span, act_bot, blk_w[2])
    with jax.named_scope("w_end"):
        pl.when(has_up)(cond_up.wait_send)
        pl.when(has_down)(cond_down.wait_send)
        drain(lat_pix.at[: (n - 1) * frames_dev], send.at[2])
        drain(res_out.at[: n - 1], send.at[3])
        drain(att_out.at[:, : n - 1], send.at[4])
        pl.when(has_up)(lambda: drain(act_out.at[0], send.at[5]))
        pl.when(has_down)(lambda: drain(act_out.at[1], send.at[6]))


def add_up(main, tail, sums, att, out_hbm, out, sem):
    frames_dev, rows, cols, channels = out.shape
    for f in range(frames_dev):
        for r in range(rows):
            convolved = conv_row(sums[f, r].reshape(cols, -1), main, tail)
            held = att[f, r].astype(F32).reshape(cols, channels)
            out[f, r] = (held + convolved).astype(BF16)
            pltpu.make_async_copy(out.at[f, r], out_hbm.at[f, r], sem).start()
    pltpu.make_async_copy(out, out_hbm, sem).wait()


def shards(
    latents,
    condition,
    key_frames,
    propagate,
    encoder_conv,
    zero_conv,
    attention_gain,
    query_weight,
    key_weight,
    value_weight,
    output_weight,
    conv_gain,
    block_conv,
):
    frames_dev, rows, cols, channels = latents.shape
    slots = condition.shape[0]
    n = lax.axis_size("frame")
    row_total = lax.axis_size("row")
    pix = rows * cols // n
    frames = frames_dev * n
    chunk = 16 if pix % 16 == 0 else 8
    chunks = pix // chunk
    group = 8
    pieces = pix // group
    block = frames * group
    per_row = n // rows
    main = channels // 256 * 256
    tail = channels - main
    wide = 3 * (main + tail)
    lat_size = packed_size(pix, channels)
    res_size = packed_size(chunk, channels)
    cond_size = packed_size(cols, channels)
    att_size = frames_dev * (channels // 128) + frames_dev // 2
    encoding = jnp.asarray(positions(frames, channels))
    square = (channels, channels)
    dma = pltpu.SemaphoreType.DMA
    values = [
        latents.reshape(frames_dev, n, pix, channels),
        condition,
        key_frames,
        propagate,
        encoding,
        attention_gain,
        conv_gain,
        encoder_conv,
        zero_conv,
        query_weight,
        key_weight,
        value_weight,
        output_weight,
        block_conv,
    ]
    values = [pltpu.with_memory_space_constraint(v, pltpu.MemorySpace.HBM) for v in values]
    sums_shape = pltpu.VMEM((frames_dev, rows, per_row, pieces, group, wide), F32)
    att_shape = pltpu.VMEM((frames_dev, rows, per_row, pieces, group, channels), BF16)
    vmem = pl.BlockSpec(memory_space=pltpu.VMEM)
    sums, att = pl.pallas_call(
        functools.partial(kernel, n, row_total),
        out_shape=(sums_shape, att_shape),
        in_specs=[pl.BlockSpec(memory_space=pl.ANY)] * len(values),
        out_specs=(vmem, vmem),
        scratch_shapes=[
            pltpu.SMEM(key_frames.shape, jnp.int32),
            pltpu.SMEM(propagate.shape, jnp.int32),
            pltpu.VMEM((frames, channels), F32),
            pltpu.VMEM((channels,), F32),
            pltpu.VMEM((channels,), F32),
            pltpu.VMEM(condition.shape, BF16),
            pltpu.VMEM((3, channels, wide), BF16),
            pltpu.VMEM((9, channels, tail), BF16),
            pltpu.VMEM((5,) + square, BF16),
            pltpu.VMEM((3, channels, wide), BF16),
            pltpu.VMEM((9, channels, tail), BF16),
            pltpu.VMEM(square, BF16),
            pltpu.VMEM((channels, 64 * HEADS), BF16),
            pltpu.VMEM((channels, 64 * HEADS), BF16),
            pltpu.VMEM((2, block, channels), BF16),
            pltpu.VMEM((2, HEADS // 2, 2 * block, 128), BF16),
            pltpu.VMEM((2, block, 64 * HEADS), BF16),
            pltpu.VMEM((2, channels, block), BF16),
            pltpu.VMEM((2, block, 2 * block), F32),
            pltpu.VMEM((2, block, 2 * block), BF16),
            pltpu.VMEM((channels, block), F32),
            pltpu.VMEM((frames_dev, n, pix, channels), BF16),
            pltpu.VMEM((n, frames_dev, lat_size, 128), BF16),
            pltpu.VMEM((frames, lat_size, 128), BF16),
            pltpu.VMEM((n, chunks, slots, res_size, 128), BF16),
            [pltpu.VMEM((slots * n, res_size, 128), BF16) for _ in range(chunks)],
            pltpu.VMEM((frames, pix, channels), F32),
            pltpu.VMEM((pieces, n, att_size, group, 128), BF16),
            pltpu.VMEM((n, pieces, att_size, group, 128), BF16),
            pltpu.VMEM((frames_dev, rows, per_row, pieces, group, channels), BF16),
            pltpu.VMEM((2, slots, cond_size, 128), BF16),
            pltpu.VMEM((slots, cond_size, 128), BF16),
            pltpu.VMEM((slots, cond_size, 128), BF16),
            pltpu.VMEM((2, pieces, per_row, att_size, group, 128), BF16),
            pltpu.VMEM((pieces, per_row, att_size, group, 128), BF16),
            pltpu.VMEM((pieces, per_row, att_size, group, 128), BF16),
            pltpu.VMEM((slots, rows, cols, wide), F32),
            dma((12,)),
            dma((7,)),
            dma((1,)),
            dma((chunks,)),
            dma((pieces, 2)),
            dma((2,)),
            dma((2, 2)),
        ],
        compiler_params=pltpu.CompilerParams(
            collective_id=0, has_side_effects=True, vmem_limit_bytes=48 * 1024 * 1024
        ),
    )(*values)
    return pl.pallas_call(
        functools.partial(add_up, main, tail),
        out_shape=jax.ShapeDtypeStruct(latents.shape, BF16),
        in_specs=[vmem, vmem],
        out_specs=pl.BlockSpec(memory_space=pl.ANY),
        scratch_shapes=[pltpu.VMEM(latents.shape, BF16), dma],
        compiler_params=pltpu.CompilerParams(vmem_limit_bytes=4 * 1024 * 1024),
    )(sums, att)


def solution(mesh):
    placed = (
        P(("group", "frame"), "row", None, None),
        P(("group", "frame"), "row", None, None),
        P("group"),
        P("group"),
        P(),
        P(),
        P(),
        P(),
        P(),
        P(),
        P(),
        P(),
        P(),
    )
    return jax.shard_map(
        shards,
        mesh=mesh,
        in_specs=placed,
        out_specs=P(("group", "frame"), "row", None, None),
        check_vma=False,
    )
```
